32 devices in a mesh: rows: 4 (over x, core), vocab: 8 (over z, y).
Axes of the slice: x: 2, y: 2, z: 4, core: 2. Of those that a mesh axis runs over, the one named last changes fastest.
Arguments:
- draft_hidden: bfloat16 [2048, 2048], P('rows'), may hold values from -128 to 128
- teacher_hidden: bfloat16 [2048, 8192], P('rows'), may hold values from -128 to 128
- draft_head: bfloat16 [2048, 8192], P(None, 'vocab'), may hold values from -4 to 4
- teacher_head: bfloat16 [8192, 8192], P(None, ('vocab', 'rows')), may hold values from -4 to 4
- row_weight: float32 [2048], P('rows'), may hold values from 1 to 16
Outputs:
- grad_hidden: bfloat16 [2048, 2048], P('rows')
- grad_head: bfloat16 [2048, 8192], P('rows', 'vocab')
- kl_rows: float32 [2048], P('rows')
The draws below stay inside these ranges and needn't reach their ends.
All inputs are finite; a program needn't handle non-finite values.
Results may differ from the reference program's by a relative error of at most 0.0051.
Values may be sent and summed in bfloat16 or wider, within the bound.
A program may use at most 192 MiB of HBM per device.

```python
import math
import jax
import jax.numpy as jnp

D_DRAFT = 2048
D_TEACH = 8192
TOKENS = 2048
VOCAB = 8192


def make_pair(key, salt, width, spread):
    folded = jax.random.fold_in(key, salt)
    key_weight, key_state = jax.random.split(folded, 2)
    weight = spread * jnp.clip(jax.random.normal(key_weight, (width, VOCAB), jnp.float32), -6.0, 6.0)
    states = jnp.clip(jax.random.normal(key_state, (TOKENS, width), jnp.float32), -6.0, 6.0)
    return (weight, states)


def draw_draft_hidden(key, part):
    return make_pair(key, 11, D_DRAFT, 3.5 / D_DRAFT ** 0.5)[1].astype(jnp.bfloat16)


def draw_draft_head(key, part):
    return make_pair(key, 11, D_DRAFT, 3.5 / D_DRAFT ** 0.5)[0].astype(jnp.bfloat16)


def draw_teacher_hidden(key, part):
    return make_pair(key, 23, D_TEACH, 4.0 / D_TEACH ** 0.5)[1].astype(jnp.bfloat16)


def draw_teacher_head(key, part):
    return make_pair(key, 23, D_TEACH, 4.0 / D_TEACH ** 0.5)[0].astype(jnp.bfloat16)


def steps_of(own_key, shape, cuts, low, top_value):
    loudness = 1.0
    for dim, blocks in cuts:
        draws = jax.random.uniform(jax.random.fold_in(jax.random.fold_in(own_key, 6), dim), (blocks,), jnp.float32, low / len(cuts), top_value / len(cuts))
        loudness = loudness * jnp.repeat(jnp.exp(draws), shape[dim] // blocks).reshape((-1,) + (1,) * (len(shape) - 1 - dim))
    return loudness


def setup_inputs(seed: int = 0) -> dict:
    key_list = jax.random.split(jax.random.key(seed), 6)
    draft_hidden = draw_draft_hidden(jax.random.fold_in(key_list[5], 71), 0)
    teacher_hidden = draw_teacher_hidden(jax.random.fold_in(key_list[5], 71), 0)
    draft_head = draw_draft_head(jax.random.fold_in(key_list[5], 71), 0)
    teacher_head = draw_teacher_head(jax.random.fold_in(key_list[5], 71), 0)
    row_weight = jnp.clip(jnp.exp(math.log(16.0) - 2.7725887 * jax.random.uniform(key_list[4], (TOKENS,), jnp.float32) ** steps_of(key_list[4], (TOKENS,), ((0, 4),), -0.2, 0.2)), 1.0, 16.0)
    return {"draft_hidden": draft_hidden, "teacher_hidden": teacher_hidden, "draft_head": draft_head, "teacher_head": teacher_head, "row_weight": row_weight}


def log_total(logits):
    peak = jnp.max(logits, axis=1)
    return peak + jnp.log(jnp.sum(jnp.exp(logits - peak[:, None]), axis=1))


def reference(draft_hidden, teacher_hidden, draft_head, teacher_head, row_weight):
    draft_logits = jnp.dot(draft_hidden, draft_head, preferred_element_type=jnp.float32)
    teacher_logits = jnp.dot(teacher_hidden, teacher_head, preferred_element_type=jnp.float32)
    draft_lse = log_total(draft_logits)
    teacher_lse = log_total(teacher_logits)
    teacher_prob = jnp.exp(teacher_logits - teacher_lse[:, None])
    draft_prob = jnp.exp(draft_logits - draft_lse[:, None])
    kl_rows = row_weight * (jnp.sum(teacher_prob * (teacher_logits - draft_logits), axis=1) - teacher_lse + draft_lse)
    grad_logits = (row_weight[:, None] * (draft_prob - teacher_prob)).astype(jnp.bfloat16)
    grad_hidden = jnp.dot(grad_logits, draft_head.T, preferred_element_type=jnp.float32).astype(jnp.bfloat16)
    grad_head = jnp.dot(draft_hidden.T, grad_logits, preferred_element_type=jnp.float32).astype(jnp.bfloat16)
    return grad_hidden, grad_head, kl_rows
```

```python
import jax
import jax.numpy as jnp
from jax import lax
from jax.experimental import pallas as pl
from jax.experimental.pallas import tpu as pltpu
from jax.sharding import PartitionSpec as P


F32, BF16 = jnp.float32, jnp.bfloat16


def make(rows, vocab):
    cores = 2 if rows % 2 == 0 else 1
    nx = rows // cores
    ny = nx if vocab % nx == 0 else 1
    nz = vocab // ny

    def shift(array, axis, dx=0, dc=0, dy=0, dz=0):
        if axis == "rows":
            perm = [
                (x * cores + c, (x + dx) % nx * cores + (c + dc) % cores)
                for x in range(nx)
                for c in range(cores)
            ]
        else:
            perm = [
                (z * ny + y, (z + dz) % nz * ny + (y + dy) % ny)
                for z in range(nz)
                for y in range(ny)
            ]
        return lax.ppermute(array, axis, perm)

    def dot(a, b):
        return jnp.dot(a, b, preferred_element_type=F32)

    def teacher(hidden, head, row, early):
        x, core = row // cores, row % cores
        width = head.shape[1]
        unit = head.shape[0] // 4
        cuts = [(k * unit, (k + 1) * unit) for k in range(4)]
        total = {}
        for dc in range(cores):
            total[0, dc] = dot(hidden, shift(head, "rows", dc=dc) if dc else head)
        held = [head[lo:hi] for lo, hi in cuts]
        for dx in range(1, nx):
            held = [shift(h, "rows", dx=1) for h in held]
            for k, (lo, hi) in enumerate(cuts):
                if k in (0, len(cuts) - 1):
                    held[k], total, early = lax.optimization_barrier((held[k], total, early))
                part = hidden[:, lo:hi]
                for dc in range(cores):
                    piece = shift(held[k], "rows", dc=dc) if dc else held[k]
                    term = dot(part, piece)
                    total[dx, dc] = total[dx, dc] + term if k else term
        out = jnp.zeros((hidden.shape[0], width * rows), F32)
        for (dx, dc), block in total.items():
            owner = (x + nx - dx) % nx * cores + (core + cores - dc) % cores
            out = lax.dynamic_update_slice(out, block, (0, owner * width))
        return out, early

    def greet(peers):
        barrier = pltpu.get_barrier_semaphore()
        for peer in peers:
            pl.semaphore_signal(
                barrier, inc=1, device_id=peer, device_id_type=pl.DeviceIdType.MESH
            )
        pl.semaphore_wait(barrier, len(peers))

    def swap_stats(stats):
        def kernel(x_ref, out_ref, send_sem, recv_sem):
            row, me = lax.axis_index("rows"), lax.axis_index("vocab")
            peers = [(row, lax.rem(me + d, vocab)) for d in range(1, vocab)]
            greet(peers)
            copies = []
            for d, peer in enumerate(peers):
                copy = pltpu.make_async_remote_copy(
                    src_ref=x_ref,
                    dst_ref=out_ref.at[me],
                    send_sem=send_sem.at[d],
                    recv_sem=recv_sem.at[d],
                    device_id=peer,
                    device_id_type=pl.DeviceIdType.MESH,
                )
                copy.start()
                copies.append(copy)
            out_ref[me] = x_ref[...]
            for copy in copies:
                copy.wait()

        return pl.pallas_call(
            kernel,
            out_shape=jax.ShapeDtypeStruct((vocab,) + stats.shape, F32),
            in_specs=[pl.BlockSpec(memory_space=pltpu.VMEM)],
            out_specs=pl.BlockSpec(memory_space=pltpu.VMEM),
            scratch_shapes=[
                pltpu.SemaphoreType.DMA((vocab - 1,)),
                pltpu.SemaphoreType.DMA((vocab - 1,)),
            ],
            compiler_params=pltpu.CompilerParams(collective_id=0, has_side_effects=True),
        )(stats)

    def sums(grad_logits, draft_head, hidden_t):
        tokens, width = grad_logits.shape
        draft = draft_head.shape[0]
        chunks = 8
        cols, ry = draft // chunks, tokens // ny
        rz, block = ry // nz, draft // rows

        def kernel(
            gl, w, ht, out, head_out,
            ysend, yrecv, acc, zsend, zrecv, csend, crecv, hacc, xsend, xrecv,
            y1s, y1r, z1s, z1r, z2s, z2r, y2s, y2r, cs, cr, xs, xr,
        ):
            row, me = lax.axis_index("rows"), lax.axis_index("vocab")
            x, core = row // cores, lax.rem(row, cores)
            z, y = me // ny, lax.rem(me, ny)
            ypeers = [(row, z * ny + lax.rem(y + d, ny)) for d in range(1, ny)]
            zpeers = [(row, lax.rem(z + d, nz) * ny + y) for d in range(1, nz)]
            cpeers = [(x * cores + lax.rem(core + d, cores), me) for d in range(1, cores)]
            xpeers = [(lax.rem(x + d, nx) * cores + core, me) for d in range(1, nx)]

            def remote(src, dst, s, r, peer):
                return pltpu.make_async_remote_copy(
                    src_ref=src, dst_ref=dst, send_sem=s, recv_sem=r,
                    device_id=peer, device_id_type=pl.DeviceIdType.MESH,
                )

            def al(v, n):
                return pl.multiple_of(v * n, n)

            def y1(d, i):
                return remote(ysend.at[d, i], yrecv.at[d, i], y1s.at[d, i], y1r.at[d, i], ypeers[d])

            def z1(d, i):
                return remote(zsend.at[d, i], zrecv.at[d, i], z1s.at[d, i], z1r.at[d, i], zpeers[d])

            def z2(d, i):
                ref = out.at[pl.ds(al(y * nz + z, rz), rz), pl.ds(i * cols, cols)]
                return remote(ref, ref, z2s.at[d, i], z2r.at[d, i], zpeers[d])

            def y2(d, i):
                ref = out.at[pl.ds(al(y, ry), ry), pl.ds(i * cols, cols)]
                return remote(ref, ref, y2s.at[d, i], y2r.at[d, i], ypeers[d])

            def cx(d, k):
                return remote(csend.at[d, k], crecv.at[d, k], cs.at[d, k], cr.at[d, k], cpeers[d])

            def xx(d):
                return remote(xsend.at[d], xrecv.at[d], xs.at[d], xr.at[d], xpeers[d])

            def hidden_dot(part, i):
                return lax.dot_general(
                    gl[pl.ds(al(part, ry), ry), :],
                    w[pl.ds(al(i, cols), cols), :],
                    (((1,), (1,)), ((), ())),
                    preferred_element_type=F32,
                )

            def head_dot(part):
                return jnp.dot(
                    ht[pl.ds(al(part, block), block), :], gl[...], preferred_element_type=F32
                )

            greet(ypeers + zpeers + cpeers + xpeers)

            def first(i, carry):
                for d in range(ny - 1):
                    ysend[d, i] = hidden_dot(lax.rem(y + d + 1, ny), i).astype(BF16)
                    y1(d, i).start()
                return carry

            def own_part(i, carry):
                acc[i] = hidden_dot(y, i)
                return carry

            lax.fori_loop(0, chunks, first, 0)
            lax.fori_loop(0, chunks, own_part, 0)

            def core_part(k, carry):
                to = lax.rem(x + k + 1, nx) * cores
                for d in range(cores - 1):
                    csend[d, k] = head_dot(to + lax.rem(core + d + 1, cores)).astype(BF16)
                    cx(d, k).start()
                return carry

            lax.fori_loop(0, nx, core_part, 0)

            def own_head(k, carry):
                hacc[k] = head_dot(lax.rem(x + k + 1, nx) * cores + core)
                return carry

            def head_mid():
                for k in range(nx):
                    total = hacc[k]
                    for d in range(cores - 1):
                        cx(d, k).wait_recv()
                        total = total + crecv[d, k].astype(F32)
                    if k < nx - 1:
                        xsend[k] = total.astype(BF16)
                        xx(k).start()
                    else:
                        hacc[k] = total

            def head_end():
                total = hacc[nx - 1]
                for d in range(nx - 1):
                    xx(d).wait_recv()
                    total = total + xrecv[d].astype(F32)
                head_out[...] = total.astype(BF16)

            def stage_a(i):
                for d in range(ny - 1):
                    y1(d, i).wait_recv()
                    acc[i] = acc[i] + yrecv[d, i].astype(F32)
                for d in range(nz - 1):
                    to = lax.rem(z + d + 1, nz)
                    zsend[d, i] = acc[i, pl.ds(al(to, rz), rz), :].astype(BF16)
                    z1(d, i).start()

            def stage_b(i):
                total = acc[i, pl.ds(al(z, rz), rz), :]
                for d in range(nz - 1):
                    z1(d, i).wait_recv()
                    total = total + zrecv[d, i].astype(F32)
                out[pl.ds(al(y * nz + z, rz), rz), i * cols : (i + 1) * cols] = total.astype(BF16)
                for d in range(nz - 1):
                    z2(d, i).start()

            def stage_c(i):
                for d in range(nz - 1):
                    z2(d, i).wait_recv()
                for d in range(ny - 1):
                    y2(d, i).start()

            for step in range(chunks + 2):
                if step < chunks:
                    stage_a(step)
                if step == 0:
                    lax.fori_loop(0, nx, own_head, 0)
                    head_mid()
                if 1 <= step <= chunks:
                    stage_b(step - 1)
                if step >= 2:
                    stage_c(step - 2)
            head_end()
            for i in range(chunks):
                for d in range(ny - 1):
                    y2(d, i).wait_recv()
                    y1(d, i).wait_send()
                    y2(d, i).wait_send()
                for d in range(nz - 1):
                    z1(d, i).wait_send()
                    z2(d, i).wait_send()
            for k in range(nx):
                for d in range(cores - 1):
                    cx(d, k).wait_send()
            for d in range(nx - 1):
                xx(d).wait_send()

        def dma(*shape):
            return pltpu.SemaphoreType.DMA(tuple(max(n, 1) for n in shape))

        def vm(dtype, *shape):
            return pltpu.VMEM(tuple(max(n, 1) for n in shape), dtype)

        return pl.pallas_call(
            kernel,
            out_shape=(
                jax.ShapeDtypeStruct((tokens, draft), BF16),
                jax.ShapeDtypeStruct((block, width), BF16),
            ),
            in_specs=[pl.BlockSpec(memory_space=pltpu.VMEM)] * 3,
            out_specs=(pl.BlockSpec(memory_space=pltpu.VMEM),) * 2,
            scratch_shapes=[
                vm(BF16, ny - 1, chunks, ry, cols),
                vm(BF16, ny - 1, chunks, ry, cols),
                vm(F32, chunks, ry, cols),
                vm(BF16, nz - 1, chunks, rz, cols),
                vm(BF16, nz - 1, chunks, rz, cols),
                vm(BF16, cores - 1, nx, block, width),
                vm(BF16, cores - 1, nx, block, width),
                vm(F32, nx, block, width),
                vm(BF16, nx - 1, block, width),
                vm(BF16, nx - 1, block, width),
            ]
            + [dma(ny - 1, chunks)] * 2
            + [dma(nz - 1, chunks)] * 4
            + [dma(ny - 1, chunks)] * 2
            + [dma(cores - 1, nx)] * 2
            + [dma(nx - 1)] * 2,
            compiler_params=pltpu.CompilerParams(
                collective_id=1, has_side_effects=True, vmem_limit_bytes=56 * 1024 * 1024
            ),
        )(grad_logits, draft_head, hidden_t)

    def fused(th, tw, hd, wd, rw):
        tokens, depth = th.shape
        wc, (draft, width) = tw.shape[1], wd.shape
        groups, pieces = 4, 8
        total = groups * pieces
        gr = tokens // groups
        pr = gr // pieces
        edge = depth // 128 // 3 * 128
        mid = depth - 2 * edge
        kc, ke, kq = depth // total, depth // pieces, depth // groups
        half = cores * wc
        dq = width // groups
        sub = gr // ny
        rz = sub // nz
        halves = 2
        hc = draft // halves
        chunks = groups * halves
        block = draft // rows

        def kernel(
            th, tw, hd, wd, rw, out, head_out, kl,
            hown, hrecv, wv, hdv, wdv, ht, dl, to, tx, es, er, ss, sr, vs, vr, cols, gl,
            ysend, yrecv, acc, zsend, zrecv, csend, crecv, hacc, xsend, xrecv,
            lw, lh, ld, ws, wr, pxs, pxr, pys, pyr, pzs, pzr, ess, esr, sss, ssr, vss, vsr,
            y1s, y1r, z1s, z1r, z2s, z2r, y2s, y2r, cs, cr, xs, xr,
        ):
            row, me = lax.axis_index("rows"), lax.axis_index("vocab")
            x, core = row // cores, lax.rem(row, cores)
            z, y = me // ny, lax.rem(me, ny)
            par = lax.rem(z, 2)
            xo, yo, co = 1 - x, 1 - y, 1 - core
            xpeer = (xo * cores + core, me)
            cpeer = (x * cores + co, me)
            ypeer = (row, z * ny + yo)
            ppeer = (row, (z + 1 - 2 * par) * ny + y)
            vpeers = [(row, lax.rem(me + d, vocab)) for d in range(1, vocab)]
            zpeers = [(row, lax.rem(z + d, nz) * ny + y) for d in range(1, nz)]

            def remote(src, dst, s, r, peer):
                return pltpu.make_async_remote_copy(
                    src_ref=src, dst_ref=dst, send_sem=s, recv_sem=r,
                    device_id=peer, device_id_type=pl.DeviceIdType.MESH,
                )

            def al(v, n):
                return pl.multiple_of(v * n, n)

            def load_w(q):
                k = pl.ds(al(q, kq), kq)
                return pltpu.make_async_copy(tw.at[k], wv.at[core, k], lw.at[q])

            def load_h(q):
                k = pl.ds(al(q, kq), kq)
                return pltpu.make_async_copy(th.at[:, k], hown.at[:, k], lh.at[q])

            def swap_w(q):
                k = pl.ds(al(q, kq), kq)
                return remote(tw.at[k], wv.at[core, k], ws.at[q], wr.at[q], cpeer)

            def edge_at(p):
                return pl.ds(al(p * ((edge + mid) // 128), 128), edge)

            def piece(ref, j, k):
                return ref.at[pl.ds(al(j, pr), pr), k]

            mid_at = pl.ds(edge, mid)

            def px(j, k):
                return remote(piece(th, j, k), piece(hrecv, j, k), pxs.at[j], pxr.at[j], xpeer)

            def py(j, k):
                ref = piece(hrecv, j, k)
                return remote(ref, ref, pys.at[j], pyr.at[j], ypeer)

            def pz(j, k):
                ref = piece(hrecv, j, k)
                return remote(ref, ref, pzs.at[j], pzr.at[j], ppeer)

            def group(g):
                return pl.ds(al(g, gr), gr)

            def send_e(g):
                return remote(es.at[group(g)], er.at[group(g)], ess.at[g], esr.at[g], xpeer)

            def send_s(g):
                return remote(ss.at[g], sr.at[g], sss.at[g], ssr.at[g], xpeer)

            def send_v(d, g):
                return remote(vs.at[g], vr.at[me, g], vss.at[d, g], vsr.at[d, g], vpeers[d])

            def got_v(d, g):
                src = lax.rem(me + vocab - d - 1, vocab)
                return remote(vs.at[g], vr.at[src, g], vss.at[d, g], vsr.at[d, g], vpeers[d])

            own_cols = pl.ds(al(x, half), half)
            far_cols = pl.ds(al(xo, half), half)
            lane = lax.broadcasted_iota(jnp.int32, (gr, 128), 1)

            def pack(columns, base=None, at=0):
                filled = jnp.zeros((gr, 128), F32) if base is None else base
                for k, column in enumerate(columns):
                    filled = jnp.where(lane == at + k, column, filled)
                return filled

            for q in range(groups):
                load_w(q).start()
                load_h(q).start()
            load_hd = pltpu.make_async_copy(hd, hdv, ld.at[0])
            load_wd = pltpu.make_async_copy(wd, wdv, ld.at[1])
            load_hd.start()
            load_wd.start()
            greet(vpeers + [xpeer, cpeer])

            def first(j, carry):
                @pl.when(y == 0)
                def _():
                    px(j, edge_at(par)).start()

                @pl.when(y == 1)
                def _():
                    px(j, mid_at).start()

                return carry

            lax.fori_loop(0, total, first, 0)
            for q in range(groups):
                swap_w(q).start()
            to[...] = jnp.zeros_like(to)
            tx[...] = jnp.zeros_like(tx)
            load_hd.wait()
            load_wd.wait()

            def finish(g):
                t = tx[group(g), :]
                m = jnp.max(t, axis=1, keepdims=True)
                t = t - m
                e = jnp.exp(t)
                s = jnp.sum(e, axis=1, keepdims=True)
                gap = jnp.sum(e * t, axis=1, keepdims=True)
                es[group(g), :] = e.astype(BF16)
                ss[g] = pack([m, s, gap]).T[:8]
                send_e(g).start()
                send_s(g).start()

            def own_stats(g):
                d = dl[group(g), :]
                dm = jnp.max(d, axis=1, keepdims=True)
                ds = jnp.sum(jnp.exp(d - dm), axis=1, keepdims=True)
                t = to[group(g), :]
                m = jnp.max(t, axis=1, keepdims=True)
                t = t - m
                e = jnp.exp(t)
                to[group(g), :] = e
                s = jnp.sum(e, axis=1, keepdims=True)
                gap = jnp.sum(e * (t - (dl[group(g), own_cols] - dm)), axis=1, keepdims=True)
                cols[group(g), :] = pack([dm, ds, m, s, gap])

            lag = 4

            def step(j, carry):
                @pl.when(j < total)
                def _():
                    @pl.when(y == 0)
                    def _():
                        px(j, edge_at(par)).wait_recv()
                        py(j, edge_at(par)).start()
                        pz(j, edge_at(par)).start()

                    @pl.when(y == 1)
                    def _():
                        px(j, mid_at).wait_recv()
                        py(j, mid_at).start()

                @pl.when((j >= 1) & (j <= total))
                def _():
                    @pl.when(y == 0)
                    def _():
                        py(j - 1, mid_at).wait_recv()

                    @pl.when(y == 1)
                    def _():
                        py(j - 1, edge_at(par)).wait_recv()
                        pz(j - 1, edge_at(par)).start()

                @pl.when((j >= lag) & (j < total + lag))
                def _():
                    pz(j - lag, edge_at(1 - par)).wait_recv()

                @pl.when(j < total)
                def _():
                    @pl.when(j < groups)
                    def _():
                        load_w(j).wait()
                        load_h(j).wait()
                        swap_w(j).wait_recv()

                    k = pl.ds(al(j, kc), kc)
                    for p in range(cores):
                        at = slice(p * wc, (p + 1) * wc)
                        to[:, at] += jnp.dot(hown[:, k], wv[p, k, :], preferred_element_type=F32)

                    @pl.when(lax.rem(j, pieces) == 1)
                    def _():
                        at = pl.ds(al(j // pieces, dq), dq)
                        dl[:, at] = jnp.dot(hdv[...], wdv[:, at], preferred_element_type=F32)

                    @pl.when(lax.rem(j, pieces) == 4)
                    def _():
                        part = pl.ds(al(j // pieces, draft // groups), draft // groups)
                        ht[part, :] = hdv[:, part].T

                begin = pieces + lag - 1

                @pl.when(j >= begin)
                def _():
                    v = j - begin
                    g, k = v // pieces, pl.ds(al(lax.rem(v, pieces), ke), ke)
                    for p in range(cores):
                        at = slice(p * wc, (p + 1) * wc)
                        tx[group(g), at] += jnp.dot(
                            hrecv[group(g), k], wv[p, k, :], preferred_element_type=F32
                        )

                    @pl.when(lax.rem(v, pieces) == pieces - 1)
                    def _():
                        finish(g)

                @pl.when((j >= total) & (j < total + groups))
                def _():
                    own_stats(j - total)

                return carry

            lax.fori_loop(0, total + pieces + lag - 1, step, 0)

            def share(g, carry):
                send_e(g).wait_recv()
                send_s(g).wait_recv()
                packed = cols[group(g), :]
                far = dl[group(g), far_cols] - packed[:, 0:1]
                q = jnp.sum(er[group(g), :].astype(F32) * far, axis=1, keepdims=True)
                st = pack([q], packed, 5).T[:8]
                dm, ds, mo, so, go = (st[k : k + 1] for k in range(5))
                q = st[5:6]
                mx, sx, gx = (sr[g, k : k + 1] for k in range(3))
                tm = jnp.maximum(mo, mx)
                ao, ax = jnp.exp(mo - tm), jnp.exp(mx - tm)
                ts = ao * so + ax * sx
                tg = ao * (go + (mo - tm) * so) + ax * (gx - q + (mx - tm) * sx)
                vs[g] = jnp.concatenate([dm, tm, ds, ts, tg, mo, mx, mx], axis=0)
                vr[me, g] = vs[g]
                for d in range(vocab - 1):
                    send_v(d, g).start()
                return carry

            def grads(g, carry):
                for d in range(vocab - 1):
                    got_v(d, g).wait_recv()
                w = rw[:, group(g)]
                stats = [[vr[v, g, k : k + 1] for v in range(vocab)] for k in range(5)]
                dms, tms, dss, tss, tgs = stats
                dm, tm = dms[0], tms[0]
                for v in range(1, vocab):
                    dm, tm = jnp.maximum(dm, dms[v]), jnp.maximum(tm, tms[v])
                ds = ts = tg = jnp.zeros_like(dm)
                for v in range(vocab):
                    dd, tt = dms[v] - dm, tms[v] - tm
                    scale = jnp.exp(tt)
                    ds = ds + dss[v] * jnp.exp(dd)
                    ts = ts + tss[v] * scale
                    tg = tg + scale * (tgs[v] + tss[v] * (tt - dd))
                kl[:, group(g)] = w * (tg / ts - jnp.log(ts) + jnp.log(ds))
                fo = w * jnp.exp(vs[g, 5:6] - tm) / ts
                fx = w * jnp.exp(vs[g, 6:7] - tm) / ts
                rows_of = jnp.concatenate([dm, w / ds, fo, fx] + [dm] * 4, axis=0)
                turned = jnp.concatenate([rows_of] * (128 // 8), axis=0).T
                dm, fd, fo, fx = (turned[:, k : k + 1] for k in range(4))
                own = fd * jnp.exp(dl[group(g), own_cols] - dm) - fo * to[group(g), :]
                gl[group(g), own_cols] = own.astype(BF16)
                far = fd * jnp.exp(dl[group(g), far_cols] - dm) - fx * er[group(g), :].astype(F32)
                gl[group(g), far_cols] = far.astype(BF16)
                return carry

            def rows_at(g, r, n):
                return pl.ds(pl.multiple_of(g * gr + r * n, n), n)

            def cols_at(h):
                return pl.ds(al(h, hc), hc)

            def y1(i):
                return remote(ysend.at[i], yrecv.at[i], y1s.at[i], y1r.at[i], ypeer)

            def z1(d, i):
                return remote(zsend.at[d, i], zrecv.at[d, i], z1s.at[d, i], z1r.at[d, i], zpeers[d])

            def z2(d, i, who):
                g, h = i // halves, lax.rem(i, halves)
                ref = out.at[rows_at(g, y * nz + who, rz), cols_at(h)]
                return remote(ref, ref, z2s.at[d, i], z2r.at[d, i], zpeers[d])

            def y2(i, who):
                g, h = i // halves, lax.rem(i, halves)
                ref = out.at[rows_at(g, who, sub), cols_at(h)]
                return remote(ref, ref, y2s.at[i], y2r.at[i], ypeer)

            def cx(k):
                return remote(csend.at[k], crecv.at[k], cs.at[k], cr.at[k], cpeer)

            def xx():
                return remote(xsend, xrecv, xs.at[0], xr.at[0], xpeer)

            def hidden(i, carry):
                g, h = i // halves, lax.rem(i, halves)
                acc[i] = lax.dot_general(
                    gl[group(g), :], wdv[cols_at(h), :],
                    (((1,), (1,)), ((), ())), preferred_element_type=F32,
                )
                ysend[i] = acc[i, pl.ds(al(yo, sub), sub), :].astype(BF16)
                y1(i).start()
                return carry

            def head_dot(part):
                return jnp.dot(
                    ht[pl.ds(al(part, block), block), :], gl[...], preferred_element_type=F32
                )

            def core_part(k, carry):
                to_chip = lax.rem(x + k + 1, nx) * cores
                csend[k] = head_dot(to_chip + co).astype(BF16)
                cx(k).start()
                return carry

            def own_head(k, carry):
                hacc[k] = head_dot(lax.rem(x + k + 1, nx) * cores + core)
                return carry

            def head_mid():
                cx(0).wait_recv()
                xsend[...] = (hacc[0] + crecv[0].astype(F32)).astype(BF16)
                xx().start()
                cx(1).wait_recv()
                hacc[1] = hacc[1] + crecv[1].astype(F32)

            def head_end():
                xx().wait_recv()
                head_out[...] = (hacc[1] + xrecv[...].astype(F32)).astype(BF16)

            def stage_a(i):
                y1(i).wait_recv()
                for d in range(nz - 1):
                    to_z = lax.rem(z + d + 1, nz)
                    mine = acc[i, pl.ds(al(y * nz + to_z, rz), rz), :]
                    mine = mine + yrecv[i, pl.ds(al(to_z, rz), rz), :].astype(F32)
                    zsend[d, i] = mine.astype(BF16)
                    z1(d, i).start()

            def stage_b(i):
                g, h = i // halves, lax.rem(i, halves)
                mine = acc[i, pl.ds(al(y * nz + z, rz), rz), :]
                mine = mine + yrecv[i, pl.ds(al(z, rz), rz), :].astype(F32)
                for d in range(nz - 1):
                    z1(d, i).wait_recv()
                    mine = mine + zrecv[d, i].astype(F32)
                out[rows_at(g, y * nz + z, rz), cols_at(h)] = mine.astype(BF16)
                for d in range(nz - 1):
                    z2(d, i, z).start()

            def stage_c(i):
                for d in range(nz - 1):
                    z2(d, i, lax.rem(z + nz - d - 1, nz)).wait_recv()
                y2(i, y).start()

            lax.fori_loop(0, groups, share, 0)

            def gradients(g, carry):
                grads(g, carry)
                lax.fori_loop(g * halves, g * halves + halves, hidden, 0)
                return carry

            lax.fori_loop(0, groups, gradients, 0)
            lax.fori_loop(0, nx, core_part, 0)

            def reduce(s, carry):
                @pl.when(s < chunks)
                def _():
                    stage_a(s)

                @pl.when(s == 0)
                def _():
                    lax.fori_loop(0, nx, own_head, 0)
                    head_mid()

                @pl.when((s >= 1) & (s <= chunks))
                def _():
                    stage_b(s - 1)

                @pl.when(s >= 2)
                def _():
                    stage_c(s - 2)

                return carry

            lax.fori_loop(0, chunks + 2, reduce, 0)
            head_end()

            def drain_out(i, carry):
                y2(i, yo).wait_recv()
                y1(i).wait_send()
                y2(i, y).wait_send()
                for d in range(nz - 1):
                    z1(d, i).wait_send()
                    z2(d, i, z).wait_send()
                return carry

            lax.fori_loop(0, chunks, drain_out, 0)
            for k in range(nx):
                cx(k).wait_send()
            xx().wait_send()

            def drain_in(j, carry):
                @pl.when(y == 0)
                def _():
                    px(j, edge_at(par)).wait_send()
                    py(j, edge_at(par)).wait_send()

                @pl.when(y == 1)
                def _():
                    px(j, mid_at).wait_send()
                    py(j, mid_at).wait_send()

                pz(j, edge_at(par)).wait_send()
                return carry

            lax.fori_loop(0, total, drain_in, 0)

            def drain_stats(g, carry):
                swap_w(g).wait_send()
                send_e(g).wait_send()
                send_s(g).wait_send()
                for d in range(vocab - 1):
                    send_v(d, g).wait_send()
                return carry

            lax.fori_loop(0, groups, drain_stats, 0)

        def dma(*shape):
            return pltpu.SemaphoreType.DMA(tuple(shape))

        anywhere = pl.BlockSpec(memory_space=pl.ANY)
        vmem = pl.BlockSpec(memory_space=pltpu.VMEM)
        return pl.pallas_call(
            kernel,
            out_shape=(
                jax.ShapeDtypeStruct((tokens, draft), BF16),
                jax.ShapeDtypeStruct((block, width), BF16),
                jax.ShapeDtypeStruct((1, tokens), F32),
            ),
            in_specs=[anywhere] * 4 + [vmem],
            out_specs=(vmem,) * 3,
            scratch_shapes=[
                pltpu.VMEM((tokens, depth), BF16),
                pltpu.VMEM((tokens, depth), BF16),
                pltpu.VMEM((cores, depth, wc), BF16),
                pltpu.VMEM((tokens, draft), BF16),
                pltpu.VMEM((draft, width), BF16),
                pltpu.VMEM((draft, tokens), BF16),
                pltpu.VMEM((tokens, width), F32),
                pltpu.VMEM((tokens, half), F32),
                pltpu.VMEM((tokens, half), F32),
                pltpu.VMEM((tokens, half), BF16),
                pltpu.VMEM((tokens, half), BF16),
                pltpu.VMEM((groups, 8, gr), F32),
                pltpu.VMEM((groups, 8, gr), F32),
                pltpu.VMEM((groups, 8, gr), F32),
                pltpu.VMEM((vocab, groups, 8, gr), F32),
                pltpu.VMEM((tokens, 128), F32),
                pltpu.VMEM((tokens, width), BF16),
                pltpu.VMEM((chunks, sub, hc), BF16),
                pltpu.VMEM((chunks, sub, hc), BF16),
                pltpu.VMEM((chunks, gr, hc), F32),
                pltpu.VMEM((nz - 1, chunks, rz, hc), BF16),
                pltpu.VMEM((nz - 1, chunks, rz, hc), BF16),
                pltpu.VMEM((nx, block, width), BF16),
                pltpu.VMEM((nx, block, width), BF16),
                pltpu.VMEM((nx, block, width), F32),
                pltpu.VMEM((block, width), BF16),
                pltpu.VMEM((block, width), BF16),
            ]
            + [dma(groups), dma(groups), dma(2), dma(groups), dma(groups)]
            + [dma(total)] * 6
            + [dma(groups)] * 4
            + [dma(vocab - 1, groups)] * 2
            + [dma(chunks)] * 2
            + [dma(nz - 1, chunks)] * 4
            + [dma(chunks)] * 2
            + [dma(nx)] * 2
            + [dma(1)] * 2,
            compiler_params=pltpu.CompilerParams(
                collective_id=2, has_side_effects=True, vmem_limit_bytes=63 * 1024 * 1024
            ),
        )(th, tw, hd, wd, rw)

    def fits(th, tw, hd, wd):
        tokens, depth = th.shape
        paired = cores == 2 and nx == 2 and ny == 2 and nz % 2 == 0
        tiled = tokens == 4 * 128 and 128 % (ny * nz * 16) == 0 and depth % 4096 == 0
        room = tokens * depth * 4 + cores * depth * tw.shape[1] * 2 <= 24 * 2**20
        return paired and tiled and room

    def gathered(draft_hidden, teacher_hidden, draft_head, teacher_head, row_weight):
        grad_hidden, grad_head, kl = fused(
            teacher_hidden, teacher_head, draft_hidden, draft_head, row_weight.reshape(1, -1)
        )
        return (grad_hidden, grad_head, kl.reshape(-1))

    def on_device(draft_hidden, teacher_hidden, draft_head, teacher_head, row_weight):
        if fits(teacher_hidden, teacher_head, draft_hidden, draft_head):
            return gathered(draft_hidden, teacher_hidden, draft_head, teacher_head, row_weight)
        row = lax.axis_index("rows")
        draft_logits = dot(draft_hidden, draft_head)
        draft_top = jnp.max(draft_logits, axis=1)
        draft_sum = jnp.sum(jnp.exp(draft_logits - draft_top[:, None]), axis=1)
        early = (draft_logits, draft_top, draft_sum, draft_hidden.T)
        teacher_logits, early = teacher(teacher_hidden, teacher_head, row, early)
        draft_logits, draft_top, draft_sum, hidden_t = early
        teach_top = jnp.max(teacher_logits, axis=1)
        teach_exp = jnp.exp(teacher_logits - teach_top[:, None])
        stats = jnp.stack(
            [
                draft_top,
                teach_top,
                draft_sum,
                jnp.sum(teach_exp, axis=1),
                jnp.sum(teach_exp * (teacher_logits - draft_logits), axis=1),
            ]
        )
        stats = swap_stats(stats)
        draft_top, teach_top = jnp.max(stats[:, 0], axis=0), jnp.max(stats[:, 1], axis=0)
        draft_scale = jnp.exp(stats[:, 0] - draft_top)
        teach_scale = jnp.exp(stats[:, 1] - teach_top)
        draft_sum = jnp.sum(stats[:, 2] * draft_scale, axis=0)
        teach_sum = jnp.sum(stats[:, 3] * teach_scale, axis=0)
        teach_gap = jnp.sum(stats[:, 4] * teach_scale, axis=0)
        draft_lse = draft_top + jnp.log(draft_sum)
        teacher_lse = teach_top + jnp.log(teach_sum)
        kl_rows = row_weight * (teach_gap / teach_sum - teacher_lse + draft_lse)
        teacher_prob = jnp.exp(teacher_logits - teacher_lse[:, None])
        draft_prob = jnp.exp(draft_logits - draft_lse[:, None])
        grad_logits = (row_weight[:, None] * (draft_prob - teacher_prob)).astype(BF16)
        grad_hidden, grad_head = sums(grad_logits, draft_head, hidden_t)
        return (grad_hidden, grad_head, kl_rows)

    return on_device


def solution(mesh):
    return jax.shard_map(
        make(mesh.shape["rows"], mesh.shape["vocab"]),
        mesh=mesh,
        in_specs=(
            P("rows", None),
            P("rows", None),
            P(None, "vocab"),
            P(None, ("vocab", "rows")),
            P("rows"),
        ),
        out_specs=(P("rows", None), P("rows", "vocab"), P("rows")),
        check_vma=False,
    )
```

```python
import jax
import jax.numpy as jnp
from jax import lax
from jax.experimental import pallas as pl
from jax.experimental.pallas import tpu as pltpu
from jax.sharding import PartitionSpec as P


F32, BF16 = jnp.float32, jnp.bfloat16


def make(rows, vocab):
    cores = 2 if rows % 2 == 0 else 1
    nx = rows // cores
    ny = nx if vocab % nx == 0 else 1
    nz = vocab // ny

    def shift(array, axis, dx=0, dc=0, dy=0, dz=0):
        if axis == "rows":
            perm = [
                (x * cores + c, (x + dx) % nx * cores + (c + dc) % cores)
                for x in range(nx)
                for c in range(cores)
            ]
        else:
            perm = [
                (z * ny + y, (z + dz) % nz * ny + (y + dy) % ny)
                for z in range(nz)
                for y in range(ny)
            ]
        return lax.ppermute(array, axis, perm)

    def dot(a, b):
        return jnp.dot(a, b, preferred_element_type=F32)

    def teacher(hidden, head, row, early):
        x, core = row // cores, row % cores
        width = head.shape[1]
        unit = head.shape[0] // 4
        cuts = [(k * unit, (k + 1) * unit) for k in range(4)]
        total = {}
        for dc in range(cores):
            total[0, dc] = dot(hidden, shift(head, "rows", dc=dc) if dc else head)
        held = [head[lo:hi] for lo, hi in cuts]
        for dx in range(1, nx):
            held = [shift(h, "rows", dx=1) for h in held]
            for k, (lo, hi) in enumerate(cuts):
                if k in (0, len(cuts) - 1):
                    held[k], total, early = lax.optimization_barrier((held[k], total, early))
                part = hidden[:, lo:hi]
                for dc in range(cores):
                    piece = shift(held[k], "rows", dc=dc) if dc else held[k]
                    term = dot(part, piece)
                    total[dx, dc] = total[dx, dc] + term if k else term
        out = jnp.zeros((hidden.shape[0], width * rows), F32)
        for (dx, dc), block in total.items():
            owner = (x + nx - dx) % nx * cores + (core + cores - dc) % cores
            out = lax.dynamic_update_slice(out, block, (0, owner * width))
        return out, early

    def greet(peers):
        barrier = pltpu.get_barrier_semaphore()
        for peer in peers:
            pl.semaphore_signal(
                barrier, inc=1, device_id=peer, device_id_type=pl.DeviceIdType.MESH
            )
        pl.semaphore_wait(barrier, len(peers))

    def swap_stats(stats):
        def kernel(x_ref, out_ref, send_sem, recv_sem):
            row, me = lax.axis_index("rows"), lax.axis_index("vocab")
            peers = [(row, lax.rem(me + d, vocab)) for d in range(1, vocab)]
            greet(peers)
            copies = []
            for d, peer in enumerate(peers):
                copy = pltpu.make_async_remote_copy(
                    src_ref=x_ref,
                    dst_ref=out_ref.at[me],
                    send_sem=send_sem.at[d],
                    recv_sem=recv_sem.at[d],
                    device_id=peer,
                    device_id_type=pl.DeviceIdType.MESH,
                )
                copy.start()
                copies.append(copy)
            out_ref[me] = x_ref[...]
            for copy in copies:
                copy.wait()

        return pl.pallas_call(
            kernel,
            out_shape=jax.ShapeDtypeStruct((vocab,) + stats.shape, F32),
            in_specs=[pl.BlockSpec(memory_space=pltpu.VMEM)],
            out_specs=pl.BlockSpec(memory_space=pltpu.VMEM),
            scratch_shapes=[
                pltpu.SemaphoreType.DMA((vocab - 1,)),
                pltpu.SemaphoreType.DMA((vocab - 1,)),
            ],
            compiler_params=pltpu.CompilerParams(collective_id=0, has_side_effects=True),
        )(stats)

    def sums(grad_logits, draft_head, hidden_t):
        tokens, width = grad_logits.shape
        draft = draft_head.shape[0]
        chunks = 8
        cols, ry = draft // chunks, tokens // ny
        rz, block = ry // nz, draft // rows

        def kernel(
            gl, w, ht, out, head_out,
            ysend, yrecv, acc, zsend, zrecv, csend, crecv, hacc, xsend, xrecv,
            y1s, y1r, z1s, z1r, z2s, z2r, y2s, y2r, cs, cr, xs, xr,
        ):
            row, me = lax.axis_index("rows"), lax.axis_index("vocab")
            x, core = row // cores, lax.rem(row, cores)
            z, y = me // ny, lax.rem(me, ny)
            ypeers = [(row, z * ny + lax.rem(y + d, ny)) for d in range(1, ny)]
            zpeers = [(row, lax.rem(z + d, nz) * ny + y) for d in range(1, nz)]
            cpeers = [(x * cores + lax.rem(core + d, cores), me) for d in range(1, cores)]
            xpeers = [(lax.rem(x + d, nx) * cores + core, me) for d in range(1, nx)]

            def remote(src, dst, s, r, peer):
                return pltpu.make_async_remote_copy(
                    src_ref=src, dst_ref=dst, send_sem=s, recv_sem=r,
                    device_id=peer, device_id_type=pl.DeviceIdType.MESH,
                )

            def al(v, n):
                return pl.multiple_of(v * n, n)

            def y1(d, i):
                return remote(ysend.at[d, i], yrecv.at[d, i], y1s.at[d, i], y1r.at[d, i], ypeers[d])

            def z1(d, i):
                return remote(zsend.at[d, i], zrecv.at[d, i], z1s.at[d, i], z1r.at[d, i], zpeers[d])

            def z2(d, i):
                ref = out.at[pl.ds(al(y * nz + z, rz), rz), pl.ds(i * cols, cols)]
                return remote(ref, ref, z2s.at[d, i], z2r.at[d, i], zpeers[d])

            def y2(d, i):
                ref = out.at[pl.ds(al(y, ry), ry), pl.ds(i * cols, cols)]
                return remote(ref, ref, y2s.at[d, i], y2r.at[d, i], ypeers[d])

            def cx(d, k):
                return remote(csend.at[d, k], crecv.at[d, k], cs.at[d, k], cr.at[d, k], cpeers[d])

            def xx(d):
                return remote(xsend.at[d], xrecv.at[d], xs.at[d], xr.at[d], xpeers[d])

            def hidden_dot(part, i):
                return lax.dot_general(
                    gl[pl.ds(al(part, ry), ry), :],
                    w[pl.ds(al(i, cols), cols), :],
                    (((1,), (1,)), ((), ())),
                    preferred_element_type=F32,
                )

            def head_dot(part):
                return jnp.dot(
                    ht[pl.ds(al(part, block), block), :], gl[...], preferred_element_type=F32
                )

            greet(ypeers + zpeers + cpeers + xpeers)

            def first(i, carry):
                for d in range(ny - 1):
                    ysend[d, i] = hidden_dot(lax.rem(y + d + 1, ny), i).astype(BF16)
                    y1(d, i).start()
                return carry

            def own_part(i, carry):
                acc[i] = hidden_dot(y, i)
                return carry

            lax.fori_loop(0, chunks, first, 0)
            lax.fori_loop(0, chunks, own_part, 0)

            def core_part(k, carry):
                to = lax.rem(x + k + 1, nx) * cores
                for d in range(cores - 1):
                    csend[d, k] = head_dot(to + lax.rem(core + d + 1, cores)).astype(BF16)
                    cx(d, k).start()
                return carry

            lax.fori_loop(0, nx, core_part, 0)

            def own_head(k, carry):
                hacc[k] = head_dot(lax.rem(x + k + 1, nx) * cores + core)
                return carry

            def head_mid():
                for k in range(nx):
                    total = hacc[k]
                    for d in range(cores - 1):
                        cx(d, k).wait_recv()
                        total = total + crecv[d, k].astype(F32)
                    if k < nx - 1:
                        xsend[k] = total.astype(BF16)
                        xx(k).start()
                    else:
                        hacc[k] = total

            def head_end():
                total = hacc[nx - 1]
                for d in range(nx - 1):
                    xx(d).wait_recv()
                    total = total + xrecv[d].astype(F32)
                head_out[...] = total.astype(BF16)

            def stage_a(i):
                for d in range(ny - 1):
                    y1(d, i).wait_recv()
                    acc[i] = acc[i] + yrecv[d, i].astype(F32)
                for d in range(nz - 1):
                    to = lax.rem(z + d + 1, nz)
                    zsend[d, i] = acc[i, pl.ds(al(to, rz), rz), :].astype(BF16)
                    z1(d, i).start()

            def stage_b(i):
                total = acc[i, pl.ds(al(z, rz), rz), :]
                for d in range(nz - 1):
                    z1(d, i).wait_recv()
                    total = total + zrecv[d, i].astype(F32)
                out[pl.ds(al(y * nz + z, rz), rz), i * cols : (i + 1) * cols] = total.astype(BF16)
                for d in range(nz - 1):
                    z2(d, i).start()

            def stage_c(i):
                for d in range(nz - 1):
                    z2(d, i).wait_recv()
                for d in range(ny - 1):
                    y2(d, i).start()

            for step in range(chunks + 2):
                if step < chunks:
                    stage_a(step)
                if step == 0:
                    lax.fori_loop(0, nx, own_head, 0)
                    head_mid()
                if 1 <= step <= chunks:
                    stage_b(step - 1)
                if step >= 2:
                    stage_c(step - 2)
            head_end()
            for i in range(chunks):
                for d in range(ny - 1):
                    y2(d, i).wait_recv()
                    y1(d, i).wait_send()
                    y2(d, i).wait_send()
                for d in range(nz - 1):
                    z1(d, i).wait_send()
                    z2(d, i).wait_send()
            for k in range(nx):
                for d in range(cores - 1):
                    cx(d, k).wait_send()
            for d in range(nx - 1):
                xx(d).wait_send()

        def dma(*shape):
            return pltpu.SemaphoreType.DMA(tuple(max(n, 1) for n in shape))

        def vm(dtype, *shape):
            return pltpu.VMEM(tuple(max(n, 1) for n in shape), dtype)

        return pl.pallas_call(
            kernel,
            out_shape=(
                jax.ShapeDtypeStruct((tokens, draft), BF16),
                jax.ShapeDtypeStruct((block, width), BF16),
            ),
            in_specs=[pl.BlockSpec(memory_space=pltpu.VMEM)] * 3,
            out_specs=(pl.BlockSpec(memory_space=pltpu.VMEM),) * 2,
            scratch_shapes=[
                vm(BF16, ny - 1, chunks, ry, cols),
                vm(BF16, ny - 1, chunks, ry, cols),
                vm(F32, chunks, ry, cols),
                vm(BF16, nz - 1, chunks, rz, cols),
                vm(BF16, nz - 1, chunks, rz, cols),
                vm(BF16, cores - 1, nx, block, width),
                vm(BF16, cores - 1, nx, block, width),
                vm(F32, nx, block, width),
                vm(BF16, nx - 1, block, width),
                vm(BF16, nx - 1, block, width),
            ]
            + [dma(ny - 1, chunks)] * 2
            + [dma(nz - 1, chunks)] * 4
            + [dma(ny - 1, chunks)] * 2
            + [dma(cores - 1, nx)] * 2
            + [dma(nx - 1)] * 2,
            compiler_params=pltpu.CompilerParams(
                collective_id=1, has_side_effects=True, vmem_limit_bytes=56 * 1024 * 1024
            ),
        )(grad_logits, draft_head, hidden_t)

    def fused(th, tw, hd, wd, rw):
        tokens, depth = th.shape
        wc, (draft, width) = tw.shape[1], wd.shape
        groups, pieces = 4, 8
        total = groups * pieces
        gr = tokens // groups
        pr = gr // pieces
        edge = depth // 128 // 3 * 128
        mid = depth - 2 * edge
        kc, ke, kq = 2 * depth // total, depth // pieces, depth // groups
        half = cores * wc
        dq = width // groups
        sub = gr // ny
        rz = sub // nz
        halves = 2
        hc = draft // halves
        chunks = groups * halves
        block = draft // rows

        def kernel(
            th, tw, hd, wd, rw, out, head_out, kl,
            hown, hrecv, wv, hdv, wdv, ht, dl, to, tx, es, er, ss, sr, vs, vr, cols, gl,
            ysend, yrecv, acc, zsend, zrecv, csend, crecv, hacc, xsend, xrecv,
            lw, lh, ld, ws, wr, pxs, pxr, pys, pyr, pzs, pzr, ess, esr, sss, ssr, vss, vsr,
            y1s, y1r, z1s, z1r, z2s, z2r, y2s, y2r, cs, cr, xs, xr,
        ):
            row, me = lax.axis_index("rows"), lax.axis_index("vocab")
            x, core = row // cores, lax.rem(row, cores)
            z, y = me // ny, lax.rem(me, ny)
            par = lax.rem(z, 2)
            xo, yo, co = 1 - x, 1 - y, 1 - core
            xpeer = (xo * cores + core, me)
            cpeer = (x * cores + co, me)
            ypeer = (row, z * ny + yo)
            pair, skip = z + 1 - 2 * par, lax.rem(z + 2, nz)
            ppeer = (row, pair * ny + y)
            qpeer = (row, skip * ny + y)
            vpeers = [(row, lax.rem(me + d, vocab)) for d in range(1, vocab)]
            zpeers = [(row, lax.rem(z + d, nz) * ny + y) for d in range(1, nz)]

            def remote(src, dst, s, r, peer):
                return pltpu.make_async_remote_copy(
                    src_ref=src, dst_ref=dst, send_sem=s, recv_sem=r,
                    device_id=peer, device_id_type=pl.DeviceIdType.MESH,
                )

            def al(v, n):
                return pl.multiple_of(v * n, n)

            def load_w(q):
                k = pl.ds(al(q, kq), kq)
                return pltpu.make_async_copy(tw.at[k], wv.at[core, k], lw.at[q])

            def load_h(q):
                k = pl.ds(al(q, kq), kq)
                return pltpu.make_async_copy(th.at[:, k], hown.at[:, k], lh.at[q])

            def swap_w(q):
                k = pl.ds(al(q, kq), kq)
                return remote(tw.at[k], wv.at[core, k], ws.at[q], wr.at[q], cpeer)

            def edge_at(p):
                return pl.ds(al(p * ((edge + mid) // 128), 128), edge)

            def piece(ref, j, k):
                return ref.at[pl.ds(al(j, pr), pr), k]

            mid_at = pl.ds(edge, mid)

            def px(j, k):
                return remote(piece(th, j, k), piece(hrecv, j, k), pxs.at[j], pxr.at[j], xpeer)

            def py(j, k):
                ref = piece(hrecv, j, k)
                return remote(ref, ref, pys.at[j], pyr.at[j], ypeer)

            def pz(j, k):
                ref = piece(hrecv, j, k)
                return remote(ref, ref, pzs.at[j], pzr.at[j], ppeer)

            def group(g):
                return pl.ds(al(g, gr), gr)

            def send_e(g):
                return remote(es.at[group(g)], er.at[group(g)], ess.at[g], esr.at[g], xpeer)

            def send_s(g):
                return remote(ss.at[g], sr.at[g], sss.at[g], ssr.at[g], xpeer)

            def send_v(d, g):
                return remote(vs.at[g], vr.at[me, g], vss.at[d, g], vsr.at[d, g], vpeers[d])

            def got_v(d, g):
                src = lax.rem(me + vocab - d - 1, vocab)
                return remote(vs.at[g], vr.at[src, g], vss.at[d, g], vsr.at[d, g], vpeers[d])

            own_cols = pl.ds(al(x, half), half)
            far_cols = pl.ds(al(xo, half), half)
            lane = lax.broadcasted_iota(jnp.int32, (gr, 128), 1)

            def pack(columns, base=None, at=0):
                filled = jnp.zeros((gr, 128), F32) if base is None else base
                for k, column in enumerate(columns):
                    filled = jnp.where(lane == at + k, column, filled)
                return filled

            for q in range(groups):
                load_w(q).start()
                load_h(q).start()
            load_hd = pltpu.make_async_copy(hd, hdv, ld.at[0])
            load_wd = pltpu.make_async_copy(wd, wdv, ld.at[1])
            load_hd.start()
            load_wd.start()
            greet(vpeers + [xpeer, cpeer])

            ahead = 6

            def first(j, carry):
                @pl.when(y == 0)
                def _():
                    px(j, edge_at(par)).start()

                @pl.when(y == 1)
                def _():
                    px(j, mid_at).start()

                return carry

            lax.fori_loop(0, ahead, first, 0)
            for q in range(groups):
                swap_w(q).start()
            to[...] = jnp.zeros_like(to)
            tx[...] = jnp.zeros_like(tx)
            load_hd.wait()
            load_wd.wait()

            def finish(g):
                t = tx[group(g), :]
                m = jnp.max(t, axis=1, keepdims=True)
                t = t - m
                e = jnp.exp(t)
                s = jnp.sum(e, axis=1, keepdims=True)
                gap = jnp.sum(e * t, axis=1, keepdims=True)
                es[group(g), :] = e.astype(BF16)
                ss[g] = pack([m, s, gap]).T[:8]
                send_e(g).start()
                send_s(g).start()

            def own_stats(g):
                d = dl[group(g), :]
                dm = jnp.max(d, axis=1, keepdims=True)
                ds = jnp.sum(jnp.exp(d - dm), axis=1, keepdims=True)
                t = to[group(g), :]
                m = jnp.max(t, axis=1, keepdims=True)
                t = t - m
                e = jnp.exp(t)
                to[group(g), :] = e
                s = jnp.sum(e, axis=1, keepdims=True)
                gap = jnp.sum(e * (t - (dl[group(g), own_cols] - dm)), axis=1, keepdims=True)
                cols[group(g), :] = pack([dm, ds, m, s, gap])

            ylag, zlag = 3, 8

            def step(j, carry):
                @pl.when(j + ahead < total)
                def _():
                    first(j + ahead, 0)

                @pl.when(j < total)
                def _():
                    @pl.when(y == 0)
                    def _():
                        px(j, edge_at(par)).wait_recv()
                        py(j, edge_at(par)).start()
                        pz(j, edge_at(par)).start()

                    @pl.when(y == 1)
                    def _():
                        px(j, mid_at).wait_recv()
                        py(j, mid_at).start()

                @pl.when((j >= ylag) & (j < total + ylag))
                def _():
                    @pl.when(y == 0)
                    def _():
                        py(j - ylag, mid_at).wait_recv()

                    @pl.when(y == 1)
                    def _():
                        py(j - ylag, edge_at(par)).wait_recv()
                        pz(j - ylag, edge_at(par)).start()

                @pl.when((j >= zlag) & (j < total + zlag))
                def _():
                    pz(j - zlag, edge_at(1 - par)).wait_recv()

                @pl.when(j < total)
                def _():
                    @pl.when(j < groups)
                    def _():
                        load_w(j).wait()
                        load_h(j).wait()
                        swap_w(j).wait_recv()

                @pl.when(j < total // 2)
                def _():
                    k = pl.ds(al(j, kc), kc)
                    for p in range(cores):
                        at = slice(p * wc, (p + 1) * wc)
                        to[:, at] += jnp.dot(hown[:, k], wv[p, k, :], preferred_element_type=F32)

                    @pl.when((j < pieces) & (lax.rem(j, 2) == 1))
                    def _():
                        at = pl.ds(al(j // 2, dq), dq)
                        dl[:, at] = jnp.dot(hdv[...], wdv[:, at], preferred_element_type=F32)

                    @pl.when((j >= pieces) & (lax.rem(j, 2) == 0))
                    def _():
                        part = pl.ds(al((j - pieces) // 2, draft // groups), draft // groups)
                        ht[part, :] = hdv[:, part].T

                @pl.when((j >= total // 2) & (j < total // 2 + groups))
                def _():
                    own_stats(j - total // 2)

                begin = pieces + ylag - 1

                @pl.when(j >= begin)
                def _():
                    v = j - begin
                    g, n = v // pieces, lax.rem(v, pieces)
                    k = pl.ds(al(n + par * (pieces - 1 - 2 * n), ke), ke)
                    for p in range(cores):
                        at = slice(p * wc, (p + 1) * wc)
                        tx[group(g), at] += jnp.dot(
                            hrecv[group(g), k], wv[p, k, :], preferred_element_type=F32
                        )

                    @pl.when(lax.rem(v, pieces) == pieces - 1)
                    def _():
                        finish(g)

                @pl.when(j == 27)
                def _():
                    share(0)

                @pl.when(j == total)
                def _():
                    grads(0)

                @pl.when((j > total) & (j <= total + halves))
                def _():
                    hidden(j - total - 1)

                @pl.when(j == total + ylag)
                def _():
                    share(1)

                return carry

            def share(g):
                send_e(g).wait_recv()
                send_s(g).wait_recv()
                packed = cols[group(g), :]
                far = dl[group(g), far_cols] - packed[:, 0:1]
                q = jnp.sum(er[group(g), :].astype(F32) * far, axis=1, keepdims=True)
                st = pack([q], packed, 5).T[:8]
                dm, ds, mo, so, go = (st[k : k + 1] for k in range(5))
                q = st[5:6]
                mx, sx, gx = (sr[g, k : k + 1] for k in range(3))
                tm = jnp.maximum(mo, mx)
                ao, ax = jnp.exp(mo - tm), jnp.exp(mx - tm)
                ts = ao * so + ax * sx
                tg = ao * (go + (mo - tm) * so) + ax * (gx - q + (mx - tm) * sx)
                vs[g] = jnp.concatenate([dm, tm, ds, ts, tg, mo, mx, mx], axis=0)
                vr[me, g] = vs[g]
                for d in range(vocab - 1):
                    send_v(d, g).start()

            def grads(g):
                for d in range(vocab - 1):
                    got_v(d, g).wait_recv()
                w = rw[:, group(g)]
                stats = [[vr[v, g, k : k + 1] for v in range(vocab)] for k in range(5)]
                dms, tms, dss, tss, tgs = stats
                dm, tm = dms[0], tms[0]
                for v in range(1, vocab):
                    dm, tm = jnp.maximum(dm, dms[v]), jnp.maximum(tm, tms[v])
                ds = ts = tg = jnp.zeros_like(dm)
                for v in range(vocab):
                    dd, tt = dms[v] - dm, tms[v] - tm
                    scale = jnp.exp(tt)
                    ds = ds + dss[v] * jnp.exp(dd)
                    ts = ts + tss[v] * scale
                    tg = tg + scale * (tgs[v] + tss[v] * (tt - dd))
                kl[:, group(g)] = w * (tg / ts - jnp.log(ts) + jnp.log(ds))
                fo = w * jnp.exp(vs[g, 5:6] - tm) / ts
                fx = w * jnp.exp(vs[g, 6:7] - tm) / ts
                rows_of = jnp.concatenate([dm, w / ds, fo, fx] + [dm] * 4, axis=0)
                turned = jnp.concatenate([rows_of] * (128 // 8), axis=0).T
                dm, fd, fo, fx = (turned[:, k : k + 1] for k in range(4))
                own = fd * jnp.exp(dl[group(g), own_cols] - dm) - fo * to[group(g), :]
                gl[group(g), own_cols] = own.astype(BF16)
                far = fd * jnp.exp(dl[group(g), far_cols] - dm) - fx * er[group(g), :].astype(F32)
                gl[group(g), far_cols] = far.astype(BF16)

            def rows_at(g, r, n):
                return pl.ds(pl.multiple_of(g * gr + r * n, n), n)

            def cols_at(h):
                return pl.ds(al(h, hc), hc)

            def y1(i):
                return remote(ysend.at[i], yrecv.at[i], y1s.at[i], y1r.at[i], ypeer)

            def z1(d, i):
                return remote(zsend.at[d, i], zrecv.at[d, i], z1s.at[d, i], z1r.at[d, i], zpeers[d])

            def z2(d, i, who):
                g, h = i // halves, lax.rem(i, halves)
                ref = out.at[rows_at(g, y * nz + who, rz), cols_at(h)]
                peer = qpeer if d == 1 else ppeer
                return remote(ref, ref, z2s.at[d, i], z2r.at[d, i], peer)

            def y2(i, who):
                g, h = i // halves, lax.rem(i, halves)
                ref = out.at[rows_at(g, who, sub), cols_at(h)]
                return remote(ref, ref, y2s.at[i], y2r.at[i], ypeer)

            def cx(k):
                return remote(csend.at[k], crecv.at[k], cs.at[k], cr.at[k], cpeer)

            def xx():
                return remote(xsend, xrecv, xs.at[0], xr.at[0], xpeer)

            def hidden(i):
                g, h = i // halves, lax.rem(i, halves)
                acc[i] = lax.dot_general(
                    gl[group(g), :], wdv[cols_at(h), :],
                    (((1,), (1,)), ((), ())), preferred_element_type=F32,
                )
                ysend[i] = acc[i, pl.ds(al(yo, sub), sub), :].astype(BF16)
                y1(i).start()

            def head_dot(part):
                return jnp.dot(
                    ht[pl.ds(al(part, block), block), :], gl[...], preferred_element_type=F32
                )

            def core_part(k, carry):
                to_chip = lax.rem(x + k + 1, nx) * cores
                csend[k] = head_dot(to_chip + co).astype(BF16)
                cx(k).start()
                return carry

            def own_head(k, carry):
                hacc[k] = head_dot(lax.rem(x + k + 1, nx) * cores + core)
                return carry

            def head_mid():
                cx(0).wait_recv()
                xsend[...] = (hacc[0] + crecv[0].astype(F32)).astype(BF16)
                xx().start()
                cx(1).wait_recv()
                hacc[1] = hacc[1] + crecv[1].astype(F32)

            def head_end():
                xx().wait_recv()
                head_out[...] = (hacc[1] + xrecv[...].astype(F32)).astype(BF16)

            def stage_a(i):
                y1(i).wait_recv()
                for d in range(nz - 1):
                    to_z = lax.rem(z + d + 1, nz)
                    mine = acc[i, pl.ds(al(y * nz + to_z, rz), rz), :]
                    mine = mine + yrecv[i, pl.ds(al(to_z, rz), rz), :].astype(F32)
                    zsend[d, i] = mine.astype(BF16)
                    z1(d, i).start()

            def stage_b(i):
                g, h = i // halves, lax.rem(i, halves)
                mine = acc[i, pl.ds(al(y * nz + z, rz), rz), :]
                mine = mine + yrecv[i, pl.ds(al(z, rz), rz), :].astype(F32)
                for d in range(nz - 1):
                    z1(d, i).wait_recv()
                    mine = mine + zrecv[d, i].astype(F32)
                out[rows_at(g, y * nz + z, rz), cols_at(h)] = mine.astype(BF16)
                z2(1, i, z).start()
                z2(0, i, z).start()

            def stage_c(i):
                z2(1, i, skip).wait_recv()
                z2(2, i, skip).start()

            def stage_d(i):
                z2(0, i, pair).wait_recv()
                z2(2, i, lax.rem(pair + 2, nz)).wait_recv()
                y2(i, y).start()

            def pair_of(stage, g):
                def run(i, carry):
                    stage(i)
                    return carry

                lax.fori_loop(g * halves, (g + 1) * halves, run, 0)

            lax.fori_loop(0, total + pieces + ylag - 1, step, 0)
            share(2)
            pair_of(stage_a, 0)
            grads(1)
            pair_of(hidden, 1)
            share(3)
            pair_of(stage_b, 0)
            grads(2)
            pair_of(hidden, 2)
            pair_of(stage_a, 1)
            grads(3)
            pair_of(stage_c, 0)
            pair_of(hidden, 3)
            lax.fori_loop(0, nx, core_part, 0)
            pair_of(stage_b, 1)
            lax.fori_loop(0, nx, own_head, 0)
            head_mid()
            pair_of(stage_d, 0)
            pair_of(stage_a, 2)
            pair_of(stage_c, 1)
            pair_of(stage_d, 1)
            pair_of(stage_b, 2)
            pair_of(stage_a, 3)
            pair_of(stage_c, 2)
            pair_of(stage_d, 2)
            pair_of(stage_b, 3)
            pair_of(stage_c, 3)
            pair_of(stage_d, 3)
            head_end()

            def drain_out(i, carry):
                y2(i, yo).wait_recv()
                y1(i).wait_send()
                y2(i, y).wait_send()
                for d in range(nz - 1):
                    z1(d, i).wait_send()
                    z2(d, i, skip if d == 2 else z).wait_send()
                return carry

            lax.fori_loop(0, chunks, drain_out, 0)
            for k in range(nx):
                cx(k).wait_send()
            xx().wait_send()

            def drain_in(j, carry):
                @pl.when(y == 0)
                def _():
                    px(j, edge_at(par)).wait_send()
                    py(j, edge_at(par)).wait_send()

                @pl.when(y == 1)
                def _():
                    px(j, mid_at).wait_send()
                    py(j, mid_at).wait_send()

                pz(j, edge_at(par)).wait_send()
                return carry

            lax.fori_loop(0, total, drain_in, 0)

            def drain_stats(g, carry):
                swap_w(g).wait_send()
                send_e(g).wait_send()
                send_s(g).wait_send()
                for d in range(vocab - 1):
                    send_v(d, g).wait_send()
                return carry

            lax.fori_loop(0, groups, drain_stats, 0)

        def dma(*shape):
            return pltpu.SemaphoreType.DMA(tuple(shape))

        anywhere = pl.BlockSpec(memory_space=pl.ANY)
        vmem = pl.BlockSpec(memory_space=pltpu.VMEM)
        return pl.pallas_call(
            kernel,
            out_shape=(
                pltpu.VMEM((tokens, draft), BF16),
                pltpu.VMEM((block, width), BF16),
                pltpu.VMEM((1, tokens), F32),
            ),
            in_specs=[anywhere] * 4 + [vmem],
            out_specs=(vmem,) * 3,
            scratch_shapes=[
                pltpu.VMEM((tokens, depth), BF16),
                pltpu.VMEM((tokens, depth), BF16),
                pltpu.VMEM((cores, depth, wc), BF16),
                pltpu.VMEM((tokens, draft), BF16),
                pltpu.VMEM((draft, width), BF16),
                pltpu.VMEM((draft, tokens), BF16),
                pltpu.VMEM((tokens, width), F32),
                pltpu.VMEM((tokens, half), F32),
                pltpu.VMEM((tokens, half), F32),
                pltpu.VMEM((tokens, half), BF16),
                pltpu.VMEM((tokens, half), BF16),
                pltpu.VMEM((groups, 8, gr), F32),
                pltpu.VMEM((groups, 8, gr), F32),
                pltpu.VMEM((groups, 8, gr), F32),
                pltpu.VMEM((vocab, groups, 8, gr), F32),
                pltpu.VMEM((tokens, 128), F32),
                pltpu.VMEM((tokens, width), BF16),
                pltpu.VMEM((chunks, sub, hc), BF16),
                pltpu.VMEM((chunks, sub, hc), BF16),
                pltpu.VMEM((chunks, gr, hc), F32),
                pltpu.VMEM((nz - 1, chunks, rz, hc), BF16),
                pltpu.VMEM((nz - 1, chunks, rz, hc), BF16),
                pltpu.VMEM((nx, block, width), BF16),
                pltpu.VMEM((nx, block, width), BF16),
                pltpu.VMEM((nx, block, width), F32),
                pltpu.VMEM((block, width), BF16),
                pltpu.VMEM((block, width), BF16),
            ]
            + [dma(groups), dma(groups), dma(2), dma(groups), dma(groups)]
            + [dma(total)] * 6
            + [dma(groups)] * 4
            + [dma(vocab - 1, groups)] * 2
            + [dma(chunks)] * 2
            + [dma(nz - 1, chunks)] * 4
            + [dma(chunks)] * 2
            + [dma(nx)] * 2
            + [dma(1)] * 2,
            compiler_params=pltpu.CompilerParams(
                collective_id=2, has_side_effects=True, vmem_limit_bytes=59 * 1024 * 1024
            ),
        )(th, tw, hd, wd, rw)

    def settle(*arrays):
        def kernel(*refs):
            n = len(arrays)
            copies = [
                pltpu.make_async_copy(refs[k], refs[n + k], refs[2 * n].at[k]) for k in range(n)
            ]
            for copy in copies:
                copy.start()
            for copy in copies:
                copy.wait()

        return pl.pallas_call(
            kernel,
            out_shape=tuple(jax.ShapeDtypeStruct(a.shape, a.dtype) for a in arrays),
            in_specs=[pl.BlockSpec(memory_space=pltpu.VMEM)] * len(arrays),
            out_specs=(pl.BlockSpec(memory_space=pl.ANY),) * len(arrays),
            scratch_shapes=[pltpu.SemaphoreType.DMA((len(arrays),))],
            compiler_params=pltpu.CompilerParams(vmem_limit_bytes=8 * 1024 * 1024),
        )(*arrays)

    def fits(th, tw, hd, wd):
        tokens, depth = th.shape
        paired = cores == 2 and nx == 2 and ny == 2 and nz == 4
        tiled = tokens == 4 * 128 and 128 % (ny * nz * 16) == 0 and depth % 4096 == 0
        room = tokens * depth * 4 + cores * depth * tw.shape[1] * 2 <= 24 * 2**20
        return paired and tiled and room

    def gathered(draft_hidden, teacher_hidden, draft_head, teacher_head, row_weight):
        grad_hidden, grad_head, kl = fused(
            teacher_hidden, teacher_head, draft_hidden, draft_head, row_weight.reshape(1, -1)
        )
        grad_hidden, grad_head = settle(grad_hidden, grad_head)
        return (grad_hidden, grad_head, kl.reshape(-1))

    def on_device(draft_hidden, teacher_hidden, draft_head, teacher_head, row_weight):
        if fits(teacher_hidden, teacher_head, draft_hidden, draft_head):
            return gathered(draft_hidden, teacher_hidden, draft_head, teacher_head, row_weight)
        row = lax.axis_index("rows")
        draft_logits = dot(draft_hidden, draft_head)
        draft_top = jnp.max(draft_logits, axis=1)
        draft_sum = jnp.sum(jnp.exp(draft_logits - draft_top[:, None]), axis=1)
        early = (draft_logits, draft_top, draft_sum, draft_hidden.T)
        teacher_logits, early = teacher(teacher_hidden, teacher_head, row, early)
        draft_logits, draft_top, draft_sum, hidden_t = early
        teach_top = jnp.max(teacher_logits, axis=1)
        teach_exp = jnp.exp(teacher_logits - teach_top[:, None])
        stats = jnp.stack(
            [
                draft_top,
                teach_top,
                draft_sum,
                jnp.sum(teach_exp, axis=1),
                jnp.sum(teach_exp * (teacher_logits - draft_logits), axis=1),
            ]
        )
        stats = swap_stats(stats)
        draft_top, teach_top = jnp.max(stats[:, 0], axis=0), jnp.max(stats[:, 1], axis=0)
        draft_scale = jnp.exp(stats[:, 0] - draft_top)
        teach_scale = jnp.exp(stats[:, 1] - teach_top)
        draft_sum = jnp.sum(stats[:, 2] * draft_scale, axis=0)
        teach_sum = jnp.sum(stats[:, 3] * teach_scale, axis=0)
        teach_gap = jnp.sum(stats[:, 4] * teach_scale, axis=0)
        draft_lse = draft_top + jnp.log(draft_sum)
        teacher_lse = teach_top + jnp.log(teach_sum)
        kl_rows = row_weight * (teach_gap / teach_sum - teacher_lse + draft_lse)
        teacher_prob = jnp.exp(teacher_logits - teacher_lse[:, None])
        draft_prob = jnp.exp(draft_logits - draft_lse[:, None])
        grad_logits = (row_weight[:, None] * (draft_prob - teacher_prob)).astype(BF16)
        grad_hidden, grad_head = sums(grad_logits, draft_head, hidden_t)
        return (grad_hidden, grad_head, kl_rows)

    return on_device


def solution(mesh):
    return jax.shard_map(
        make(mesh.shape["rows"], mesh.shape["vocab"]),
        mesh=mesh,
        in_specs=(
            P("rows", None),
            P("rows", None),
            P(None, "vocab"),
            P(None, ("vocab", "rows")),
            P("rows"),
        ),
        out_specs=(P("rows", None), P("rows", "vocab"), P("rows")),
        check_vma=False,
    )
```

```python
import jax
import jax.numpy as jnp
from jax import lax
from jax.experimental import pallas as pl
from jax.experimental.pallas import tpu as pltpu
from jax.sharding import PartitionSpec as P


F32, BF16 = jnp.float32, jnp.bfloat16


def make(rows, vocab):
    cores = 2 if rows % 2 == 0 else 1
    nx = rows // cores
    ny = nx if vocab % nx == 0 else 1
    nz = vocab // ny

    def shift(array, axis, dx=0, dc=0, dy=0, dz=0):
        if axis == "rows":
            perm = [
                (x * cores + c, (x + dx) % nx * cores + (c + dc) % cores)
                for x in range(nx)
                for c in range(cores)
            ]
        else:
            perm = [
                (z * ny + y, (z + dz) % nz * ny + (y + dy) % ny)
                for z in range(nz)
                for y in range(ny)
            ]
        return lax.ppermute(array, axis, perm)

    def dot(a, b):
        return jnp.dot(a, b, preferred_element_type=F32)

    def teacher(hidden, head, row, early):
        x, core = row // cores, row % cores
        width = head.shape[1]
        unit = head.shape[0] // 4
        cuts = [(k * unit, (k + 1) * unit) for k in range(4)]
        total = {}
        for dc in range(cores):
            total[0, dc] = dot(hidden, shift(head, "rows", dc=dc) if dc else head)
        held = [head[lo:hi] for lo, hi in cuts]
        for dx in range(1, nx):
            held = [shift(h, "rows", dx=1) for h in held]
            for k, (lo, hi) in enumerate(cuts):
                if k in (0, len(cuts) - 1):
                    held[k], total, early = lax.optimization_barrier((held[k], total, early))
                part = hidden[:, lo:hi]
                for dc in range(cores):
                    piece = shift(held[k], "rows", dc=dc) if dc else held[k]
                    term = dot(part, piece)
                    total[dx, dc] = total[dx, dc] + term if k else term
        out = jnp.zeros((hidden.shape[0], width * rows), F32)
        for (dx, dc), block in total.items():
            owner = (x + nx - dx) % nx * cores + (core + cores - dc) % cores
            out = lax.dynamic_update_slice(out, block, (0, owner * width))
        return out, early

    def greet(peers):
        barrier = pltpu.get_barrier_semaphore()
        for peer in peers:
            pl.semaphore_signal(
                barrier, inc=1, device_id=peer, device_id_type=pl.DeviceIdType.MESH
            )
        pl.semaphore_wait(barrier, len(peers))

    def swap_stats(stats):
        def kernel(x_ref, out_ref, send_sem, recv_sem):
            row, me = lax.axis_index("rows"), lax.axis_index("vocab")
            peers = [(row, lax.rem(me + d, vocab)) for d in range(1, vocab)]
            greet(peers)
            copies = []
            for d, peer in enumerate(peers):
                copy = pltpu.make_async_remote_copy(
                    src_ref=x_ref,
                    dst_ref=out_ref.at[me],
                    send_sem=send_sem.at[d],
                    recv_sem=recv_sem.at[d],
                    device_id=peer,
                    device_id_type=pl.DeviceIdType.MESH,
                )
                copy.start()
                copies.append(copy)
            out_ref[me] = x_ref[...]
            for copy in copies:
                copy.wait()

        return pl.pallas_call(
            kernel,
            out_shape=jax.ShapeDtypeStruct((vocab,) + stats.shape, F32),
            in_specs=[pl.BlockSpec(memory_space=pltpu.VMEM)],
            out_specs=pl.BlockSpec(memory_space=pltpu.VMEM),
            scratch_shapes=[
                pltpu.SemaphoreType.DMA((vocab - 1,)),
                pltpu.SemaphoreType.DMA((vocab - 1,)),
            ],
            compiler_params=pltpu.CompilerParams(collective_id=0, has_side_effects=True),
        )(stats)

    def sums(grad_logits, draft_head, hidden_t):
        tokens, width = grad_logits.shape
        draft = draft_head.shape[0]
        chunks = 8
        cols, ry = draft // chunks, tokens // ny
        rz, block = ry // nz, draft // rows

        def kernel(
            gl, w, ht, out, head_out,
            ysend, yrecv, acc, zsend, zrecv, csend, crecv, hacc, xsend, xrecv,
            y1s, y1r, z1s, z1r, z2s, z2r, y2s, y2r, cs, cr, xs, xr,
        ):
            row, me = lax.axis_index("rows"), lax.axis_index("vocab")
            x, core = row // cores, lax.rem(row, cores)
            z, y = me // ny, lax.rem(me, ny)
            ypeers = [(row, z * ny + lax.rem(y + d, ny)) for d in range(1, ny)]
            zpeers = [(row, lax.rem(z + d, nz) * ny + y) for d in range(1, nz)]
            cpeers = [(x * cores + lax.rem(core + d, cores), me) for d in range(1, cores)]
            xpeers = [(lax.rem(x + d, nx) * cores + core, me) for d in range(1, nx)]

            def remote(src, dst, s, r, peer):
                return pltpu.make_async_remote_copy(
                    src_ref=src, dst_ref=dst, send_sem=s, recv_sem=r,
                    device_id=peer, device_id_type=pl.DeviceIdType.MESH,
                )

            def al(v, n):
                return pl.multiple_of(v * n, n)

            def y1(d, i):
                return remote(ysend.at[d, i], yrecv.at[d, i], y1s.at[d, i], y1r.at[d, i], ypeers[d])

            def z1(d, i):
                return remote(zsend.at[d, i], zrecv.at[d, i], z1s.at[d, i], z1r.at[d, i], zpeers[d])

            def z2(d, i):
                ref = out.at[pl.ds(al(y * nz + z, rz), rz), pl.ds(i * cols, cols)]
                return remote(ref, ref, z2s.at[d, i], z2r.at[d, i], zpeers[d])

            def y2(d, i):
                ref = out.at[pl.ds(al(y, ry), ry), pl.ds(i * cols, cols)]
                return remote(ref, ref, y2s.at[d, i], y2r.at[d, i], ypeers[d])

            def cx(d, k):
                return remote(csend.at[d, k], crecv.at[d, k], cs.at[d, k], cr.at[d, k], cpeers[d])

            def xx(d):
                return remote(xsend.at[d], xrecv.at[d], xs.at[d], xr.at[d], xpeers[d])

            def hidden_dot(part, i):
                return lax.dot_general(
                    gl[pl.ds(al(part, ry), ry), :],
                    w[pl.ds(al(i, cols), cols), :],
                    (((1,), (1,)), ((), ())),
                    preferred_element_type=F32,
                )

            def head_dot(part):
                return jnp.dot(
                    ht[pl.ds(al(part, block), block), :], gl[...], preferred_element_type=F32
                )

            greet(ypeers + zpeers + cpeers + xpeers)

            def first(i, carry):
                for d in range(ny - 1):
                    ysend[d, i] = hidden_dot(lax.rem(y + d + 1, ny), i).astype(BF16)
                    y1(d, i).start()
                return carry

            def own_part(i, carry):
                acc[i] = hidden_dot(y, i)
                return carry

            lax.fori_loop(0, chunks, first, 0)
            lax.fori_loop(0, chunks, own_part, 0)

            def core_part(k, carry):
                to = lax.rem(x + k + 1, nx) * cores
                for d in range(cores - 1):
                    csend[d, k] = head_dot(to + lax.rem(core + d + 1, cores)).astype(BF16)
                    cx(d, k).start()
                return carry

            lax.fori_loop(0, nx, core_part, 0)

            def own_head(k, carry):
                hacc[k] = head_dot(lax.rem(x + k + 1, nx) * cores + core)
                return carry

            def head_mid():
                for k in range(nx):
                    total = hacc[k]
                    for d in range(cores - 1):
                        cx(d, k).wait_recv()
                        total = total + crecv[d, k].astype(F32)
                    if k < nx - 1:
                        xsend[k] = total.astype(BF16)
                        xx(k).start()
                    else:
                        hacc[k] = total

            def head_end():
                total = hacc[nx - 1]
                for d in range(nx - 1):
                    xx(d).wait_recv()
                    total = total + xrecv[d].astype(F32)
                head_out[...] = total.astype(BF16)

            def stage_a(i):
                for d in range(ny - 1):
                    y1(d, i).wait_recv()
                    acc[i] = acc[i] + yrecv[d, i].astype(F32)
                for d in range(nz - 1):
                    to = lax.rem(z + d + 1, nz)
                    zsend[d, i] = acc[i, pl.ds(al(to, rz), rz), :].astype(BF16)
                    z1(d, i).start()

            def stage_b(i):
                total = acc[i, pl.ds(al(z, rz), rz), :]
                for d in range(nz - 1):
                    z1(d, i).wait_recv()
                    total = total + zrecv[d, i].astype(F32)
                out[pl.ds(al(y * nz + z, rz), rz), i * cols : (i + 1) * cols] = total.astype(BF16)
                for d in range(nz - 1):
                    z2(d, i).start()

            def stage_c(i):
                for d in range(nz - 1):
                    z2(d, i).wait_recv()
                for d in range(ny - 1):
                    y2(d, i).start()

            for step in range(chunks + 2):
                if step < chunks:
                    stage_a(step)
                if step == 0:
                    lax.fori_loop(0, nx, own_head, 0)
                    head_mid()
                if 1 <= step <= chunks:
                    stage_b(step - 1)
                if step >= 2:
                    stage_c(step - 2)
            head_end()
            for i in range(chunks):
                for d in range(ny - 1):
                    y2(d, i).wait_recv()
                    y1(d, i).wait_send()
                    y2(d, i).wait_send()
                for d in range(nz - 1):
                    z1(d, i).wait_send()
                    z2(d, i).wait_send()
            for k in range(nx):
                for d in range(cores - 1):
                    cx(d, k).wait_send()
            for d in range(nx - 1):
                xx(d).wait_send()

        def dma(*shape):
            return pltpu.SemaphoreType.DMA(tuple(max(n, 1) for n in shape))

        def vm(dtype, *shape):
            return pltpu.VMEM(tuple(max(n, 1) for n in shape), dtype)

        return pl.pallas_call(
            kernel,
            out_shape=(
                jax.ShapeDtypeStruct((tokens, draft), BF16),
                jax.ShapeDtypeStruct((block, width), BF16),
            ),
            in_specs=[pl.BlockSpec(memory_space=pltpu.VMEM)] * 3,
            out_specs=(pl.BlockSpec(memory_space=pltpu.VMEM),) * 2,
            scratch_shapes=[
                vm(BF16, ny - 1, chunks, ry, cols),
                vm(BF16, ny - 1, chunks, ry, cols),
                vm(F32, chunks, ry, cols),
                vm(BF16, nz - 1, chunks, rz, cols),
                vm(BF16, nz - 1, chunks, rz, cols),
                vm(BF16, cores - 1, nx, block, width),
                vm(BF16, cores - 1, nx, block, width),
                vm(F32, nx, block, width),
                vm(BF16, nx - 1, block, width),
                vm(BF16, nx - 1, block, width),
            ]
            + [dma(ny - 1, chunks)] * 2
            + [dma(nz - 1, chunks)] * 4
            + [dma(ny - 1, chunks)] * 2
            + [dma(cores - 1, nx)] * 2
            + [dma(nx - 1)] * 2,
            compiler_params=pltpu.CompilerParams(
                collective_id=1, has_side_effects=True, vmem_limit_bytes=56 * 1024 * 1024
            ),
        )(grad_logits, draft_head, hidden_t)

    def fused(th, tw, hd, wd, rw):
        tokens, depth = th.shape
        wc, (draft, width) = tw.shape[1], wd.shape
        groups, pieces = 4, 8
        total = groups * pieces
        gr = tokens // groups
        pr = gr // pieces
        edge = depth // 128 // 3 * 128
        mid = depth - 2 * edge
        kc, ke, kq = 2 * depth // total, depth // pieces, depth // groups
        half = cores * wc
        dq = width // groups
        sub = gr // ny
        rz = sub // nz
        halves = 2
        hc = draft // halves
        chunks = groups * halves
        block = draft // rows

        def kernel(
            th, tw, hd, wd, rw, out, head_out, kl,
            hown, hrecv, wv, hdv, wdv, ht, dl, to, tx, es, er, ss, sr, vs, vr, cols, gl,
            ysend, yrecv, acc, zsend, zrecv, csend, crecv, hacc, xsend, xrecv,
            lw, lh, ld, ws, wr, pxs, pxr, pys, pyr, pzs, pzr, ess, esr, sss, ssr, vss, vsr,
            y1s, y1r, z1s, z1r, z2s, z2r, y2s, y2r, cs, cr, xs, xr,
        ):
            row, me = lax.axis_index("rows"), lax.axis_index("vocab")
            x, core = row // cores, lax.rem(row, cores)
            z, y = me // ny, lax.rem(me, ny)
            par = lax.rem(z, 2)
            xo, yo, co = 1 - x, 1 - y, 1 - core
            xpeer = (xo * cores + core, me)
            cpeer = (x * cores + co, me)
            ypeer = (row, z * ny + yo)
            pair, skip = z + 1 - 2 * par, lax.rem(z + 2, nz)
            ppeer = (row, pair * ny + y)
            qpeer = (row, skip * ny + y)
            vpeers = [(row, lax.rem(me + d, vocab)) for d in range(1, vocab)]
            zpeers = [(row, lax.rem(z + d, nz) * ny + y) for d in range(1, nz)]

            def remote(src, dst, s, r, peer):
                return pltpu.make_async_remote_copy(
                    src_ref=src, dst_ref=dst, send_sem=s, recv_sem=r,
                    device_id=peer, device_id_type=pl.DeviceIdType.MESH,
                )

            def al(v, n):
                return pl.multiple_of(v * n, n)

            def load_w(q):
                k = pl.ds(al(q, kq), kq)
                return pltpu.make_async_copy(tw.at[k], wv.at[core, k], lw.at[q])

            def load_h(q):
                k = pl.ds(al(q, kq), kq)
                return pltpu.make_async_copy(th.at[:, k], hown.at[:, k], lh.at[q])

            def swap_w(q):
                k = pl.ds(al(q, kq), kq)
                return remote(tw.at[k], wv.at[core, k], ws.at[q], wr.at[q], cpeer)

            def edge_at(p):
                return pl.ds(al(p * ((edge + mid) // 128), 128), edge)

            def piece(ref, j, k):
                return ref.at[pl.ds(al(j, pr), pr), k]

            mid_at = pl.ds(edge, mid)

            def px(j, k):
                return remote(piece(th, j, k), piece(hrecv, j, k), pxs.at[j], pxr.at[j], xpeer)

            def py(j, k):
                ref = piece(hrecv, j, k)
                return remote(ref, ref, pys.at[j], pyr.at[j], ypeer)

            def pz(j, k):
                ref = piece(hrecv, j, k)
                return remote(ref, ref, pzs.at[j], pzr.at[j], ppeer)

            def group(g):
                return pl.ds(al(g, gr), gr)

            def send_e(g):
                return remote(es.at[group(g)], er.at[group(g)], ess.at[g], esr.at[g], xpeer)

            def send_s(g):
                return remote(ss.at[g], sr.at[g], sss.at[g], ssr.at[g], xpeer)

            def send_v(d, g):
                return remote(vs.at[g], vr.at[me, g], vss.at[d, g], vsr.at[d, g], vpeers[d])

            def got_v(d, g):
                src = lax.rem(me + vocab - d - 1, vocab)
                return remote(vs.at[g], vr.at[src, g], vss.at[d, g], vsr.at[d, g], vpeers[d])

            own_cols = pl.ds(al(x, half), half)
            far_cols = pl.ds(al(xo, half), half)
            lane = lax.broadcasted_iota(jnp.int32, (gr, 128), 1)

            def pack(columns, base=None, at=0):
                filled = jnp.zeros((gr, 128), F32) if base is None else base
                for k, column in enumerate(columns):
                    filled = jnp.where(lane == at + k, column, filled)
                return filled

            for q in range(groups):
                load_w(q).start()
                load_h(q).start()
            load_hd = pltpu.make_async_copy(hd, hdv, ld.at[0])
            load_wd = pltpu.make_async_copy(wd, wdv, ld.at[1])
            load_hd.start()
            load_wd.start()
            greet(vpeers + [xpeer, cpeer])

            ahead = 8

            def first(j, carry):
                @pl.when(y == 0)
                def _():
                    px(j, edge_at(par)).start()

                @pl.when(y == 1)
                def _():
                    px(j, mid_at).start()

                return carry

            lax.fori_loop(0, ahead, first, 0)
            for q in range(groups):
                swap_w(q).start()
            to[...] = jnp.zeros_like(to)
            tx[...] = jnp.zeros_like(tx)

            def finish(g):
                t = tx[group(g), :]
                m = jnp.max(t, axis=1, keepdims=True)
                t = t - m
                e = jnp.exp(t)
                s = jnp.sum(e, axis=1, keepdims=True)
                gap = jnp.sum(e * t, axis=1, keepdims=True)
                es[group(g), :] = e.astype(BF16)
                ss[g] = pack([m, s, gap]).T[:8]
                send_e(g).start()
                send_s(g).start()

            def own_stats(g):
                d = dl[group(g), :]
                dm = jnp.max(d, axis=1, keepdims=True)
                ds = jnp.sum(jnp.exp(d - dm), axis=1, keepdims=True)
                t = to[group(g), :]
                m = jnp.max(t, axis=1, keepdims=True)
                t = t - m
                e = jnp.exp(t)
                to[group(g), :] = e
                s = jnp.sum(e, axis=1, keepdims=True)
                gap = jnp.sum(e * (t - (dl[group(g), own_cols] - dm)), axis=1, keepdims=True)
                cols[group(g), :] = pack([dm, ds, m, s, gap])

            ylag, zlag = 3, 8

            def step(j, carry):
                @pl.when(j + ahead < total)
                def _():
                    first(j + ahead, 0)

                @pl.when(j < total)
                def _():
                    @pl.when(y == 0)
                    def _():
                        px(j, edge_at(par)).wait_recv()
                        py(j, edge_at(par)).start()
                        pz(j, edge_at(par)).start()

                    @pl.when(y == 1)
                    def _():
                        px(j, mid_at).wait_recv()
                        py(j, mid_at).start()

                @pl.when((j >= ylag) & (j < total + ylag))
                def _():
                    @pl.when(y == 0)
                    def _():
                        py(j - ylag, mid_at).wait_recv()

                    @pl.when(y == 1)
                    def _():
                        py(j - ylag, edge_at(par)).wait_recv()
                        pz(j - ylag, edge_at(par)).start()

                @pl.when((j >= zlag) & (j < total + zlag))
                def _():
                    pz(j - zlag, edge_at(1 - par)).wait_recv()

                @pl.when(j < total)
                def _():
                    @pl.when(j < groups)
                    def _():
                        load_w(j).wait()
                        load_h(j).wait()
                        swap_w(j).wait_recv()

                @pl.when(j < total // 2)
                def _():
                    k = pl.ds(al(j, kc), kc)
                    for p in range(cores):
                        at = slice(p * wc, (p + 1) * wc)
                        to[:, at] += jnp.dot(hown[:, k], wv[p, k, :], preferred_element_type=F32)

                    @pl.when(j == 1)
                    def _():
                        load_hd.wait()
                        load_wd.wait()

                    @pl.when((j < pieces) & (lax.rem(j, 2) == 1))
                    def _():
                        at = pl.ds(al(j // 2, dq), dq)
                        dl[:, at] = jnp.dot(hdv[...], wdv[:, at], preferred_element_type=F32)

                    @pl.when((j >= pieces) & (lax.rem(j, 2) == 0))
                    def _():
                        part = pl.ds(al((j - pieces) // 2, draft // groups), draft // groups)
                        ht[part, :] = hdv[:, part].T

                @pl.when((j >= total // 2) & (j < total // 2 + groups))
                def _():
                    own_stats(j - total // 2)

                begin = pieces + ylag - 1

                @pl.when(j >= begin)
                def _():
                    v = j - begin
                    g, n = v // pieces, lax.rem(v, pieces)
                    k = pl.ds(al(n + par * (pieces - 1 - 2 * n), ke), ke)
                    for p in range(cores):
                        at = slice(p * wc, (p + 1) * wc)
                        tx[group(g), at] += jnp.dot(
                            hrecv[group(g), k], wv[p, k, :], preferred_element_type=F32
                        )

                    @pl.when(lax.rem(v, pieces) == pieces - 1)
                    def _():
                        finish(g)

                @pl.when(j == 28)
                def _():
                    share(0)

                @pl.when(j == total)
                def _():
                    grads(0)

                @pl.when((j > total) & (j <= total + halves))
                def _():
                    hidden(j - total - 1)

                @pl.when(j == total + ylag)
                def _():
                    share(1)

                return carry

            def share(g):
                send_e(g).wait_recv()
                send_s(g).wait_recv()
                packed = cols[group(g), :]
                far = dl[group(g), far_cols] - packed[:, 0:1]
                q = jnp.sum(er[group(g), :].astype(F32) * far, axis=1, keepdims=True)
                st = pack([q], packed, 5).T[:8]
                dm, ds, mo, so, go = (st[k : k + 1] for k in range(5))
                q = st[5:6]
                mx, sx, gx = (sr[g, k : k + 1] for k in range(3))
                tm = jnp.maximum(mo, mx)
                ao, ax = jnp.exp(mo - tm), jnp.exp(mx - tm)
                ts = ao * so + ax * sx
                tg = ao * (go + (mo - tm) * so) + ax * (gx - q + (mx - tm) * sx)
                vs[g] = jnp.concatenate([dm, tm, ds, ts, tg, mo, mx, mx], axis=0)
                vr[me, g] = vs[g]
                for d in range(vocab - 1):
                    send_v(d, g).start()

            def grads(g):
                for d in range(vocab - 1):
                    got_v(d, g).wait_recv()
                w = rw[:, group(g)]
                stats = [[vr[v, g, k : k + 1] for v in range(vocab)] for k in range(5)]
                dms, tms, dss, tss, tgs = stats
                dm, tm = dms[0], tms[0]
                for v in range(1, vocab):
                    dm, tm = jnp.maximum(dm, dms[v]), jnp.maximum(tm, tms[v])
                ds = ts = tg = jnp.zeros_like(dm)
                for v in range(vocab):
                    dd, tt = dms[v] - dm, tms[v] - tm
                    scale = jnp.exp(tt)
                    ds = ds + dss[v] * jnp.exp(dd)
                    ts = ts + tss[v] * scale
                    tg = tg + scale * (tgs[v] + tss[v] * (tt - dd))
                kl[:, group(g)] = w * (tg / ts - jnp.log(ts) + jnp.log(ds))
                fo = w * jnp.exp(vs[g, 5:6] - tm) / ts
                fx = w * jnp.exp(vs[g, 6:7] - tm) / ts
                rows_of = jnp.concatenate([dm, w / ds, fo, fx] + [dm] * 4, axis=0)
                turned = jnp.concatenate([rows_of] * (128 // 8), axis=0).T
                dm, fd, fo, fx = (turned[:, k : k + 1] for k in range(4))
                own = fd * jnp.exp(dl[group(g), own_cols] - dm) - fo * to[group(g), :]
                gl[group(g), own_cols] = own.astype(BF16)
                far = fd * jnp.exp(dl[group(g), far_cols] - dm) - fx * er[group(g), :].astype(F32)
                gl[group(g), far_cols] = far.astype(BF16)

            def rows_at(g, r, n):
                return pl.ds(pl.multiple_of(g * gr + r * n, n), n)

            def cols_at(h):
                return pl.ds(al(h, hc), hc)

            def y1(i):
                return remote(ysend.at[i], yrecv.at[i], y1s.at[i], y1r.at[i], ypeer)

            def z1(d, i):
                return remote(zsend.at[d, i], zrecv.at[d, i], z1s.at[d, i], z1r.at[d, i], zpeers[d])

            def z2(d, i, who):
                g, h = i // halves, lax.rem(i, halves)
                ref = out.at[rows_at(g, y * nz + who, rz), cols_at(h)]
                peer = qpeer if d == 1 else ppeer
                return remote(ref, ref, z2s.at[d, i], z2r.at[d, i], peer)

            def y2(i, who):
                g, h = i // halves, lax.rem(i, halves)
                ref = out.at[rows_at(g, who, sub), cols_at(h)]
                return remote(ref, ref, y2s.at[i], y2r.at[i], ypeer)

            def cx(k):
                return remote(csend.at[k], crecv.at[k], cs.at[k], cr.at[k], cpeer)

            def xx():
                return remote(xsend, xrecv, xs.at[0], xr.at[0], xpeer)

            def hidden(i):
                g, h = i // halves, lax.rem(i, halves)
                acc[i] = lax.dot_general(
                    gl[group(g), :], wdv[cols_at(h), :],
                    (((1,), (1,)), ((), ())), preferred_element_type=F32,
                )
                ysend[i] = acc[i, pl.ds(al(yo, sub), sub), :].astype(BF16)
                y1(i).start()

            def head_dot(part):
                return jnp.dot(
                    ht[pl.ds(al(part, block), block), :], gl[...], preferred_element_type=F32
                )

            def core_part(k, carry):
                to_chip = lax.rem(x + k + 1, nx) * cores
                csend[k] = head_dot(to_chip + co).astype(BF16)
                cx(k).start()
                return carry

            def own_head(k, carry):
                hacc[k] = head_dot(lax.rem(x + k + 1, nx) * cores + core)
                return carry

            def head_mid():
                cx(0).wait_recv()
                xsend[...] = (hacc[0] + crecv[0].astype(F32)).astype(BF16)
                xx().start()
                cx(1).wait_recv()
                hacc[1] = hacc[1] + crecv[1].astype(F32)

            def head_end():
                xx().wait_recv()
                head_out[...] = (hacc[1] + xrecv[...].astype(F32)).astype(BF16)

            def stage_a(i):
                y1(i).wait_recv()
                for d in range(nz - 1):
                    to_z = lax.rem(z + d + 1, nz)
                    mine = acc[i, pl.ds(al(y * nz + to_z, rz), rz), :]
                    mine = mine + yrecv[i, pl.ds(al(to_z, rz), rz), :].astype(F32)
                    zsend[d, i] = mine.astype(BF16)
                    z1(d, i).start()

            def stage_b(i):
                g, h = i // halves, lax.rem(i, halves)
                mine = acc[i, pl.ds(al(y * nz + z, rz), rz), :]
                mine = mine + yrecv[i, pl.ds(al(z, rz), rz), :].astype(F32)
                for d in range(nz - 1):
                    z1(d, i).wait_recv()
                    mine = mine + zrecv[d, i].astype(F32)
                out[rows_at(g, y * nz + z, rz), cols_at(h)] = mine.astype(BF16)
                z2(1, i, z).start()
                z2(0, i, z).start()

            def stage_c(i):
                z2(1, i, skip).wait_recv()
                z2(2, i, skip).start()

            def stage_d(i):
                z2(0, i, pair).wait_recv()
                z2(2, i, lax.rem(pair + 2, nz)).wait_recv()
                y2(i, y).start()

            def pair_of(stage, g):
                def run(i, carry):
                    stage(i)
                    return carry

                lax.fori_loop(g * halves, (g + 1) * halves, run, 0)

            lax.fori_loop(0, total + pieces + ylag - 1, step, 0)
            share(2)
            pair_of(stage_a, 0)
            grads(1)
            pair_of(hidden, 1)
            share(3)
            pair_of(stage_b, 0)
            grads(2)
            pair_of(hidden, 2)
            pair_of(stage_a, 1)
            grads(3)
            pair_of(stage_c, 0)
            pair_of(hidden, 3)
            lax.fori_loop(0, nx, core_part, 0)
            pair_of(stage_b, 1)
            lax.fori_loop(0, nx, own_head, 0)
            head_mid()
            pair_of(stage_d, 0)
            pair_of(stage_a, 2)
            pair_of(stage_c, 1)
            pair_of(stage_d, 1)
            pair_of(stage_b, 2)
            pair_of(stage_a, 3)
            pair_of(stage_c, 2)
            pair_of(stage_d, 2)
            pair_of(stage_b, 3)
            pair_of(stage_c, 3)
            pair_of(stage_d, 3)
            head_end()

            def drain_out(i, carry):
                y2(i, yo).wait_recv()
                y1(i).wait_send()
                y2(i, y).wait_send()
                for d in range(nz - 1):
                    z1(d, i).wait_send()
                    z2(d, i, skip if d == 2 else z).wait_send()
                return carry

            lax.fori_loop(0, chunks, drain_out, 0)
            for k in range(nx):
                cx(k).wait_send()
            xx().wait_send()

            def drain_in(j, carry):
                @pl.when(y == 0)
                def _():
                    px(j, edge_at(par)).wait_send()
                    py(j, edge_at(par)).wait_send()

                @pl.when(y == 1)
                def _():
                    px(j, mid_at).wait_send()
                    py(j, mid_at).wait_send()

                pz(j, edge_at(par)).wait_send()
                return carry

            lax.fori_loop(0, total, drain_in, 0)

            def drain_stats(g, carry):
                swap_w(g).wait_send()
                send_e(g).wait_send()
                send_s(g).wait_send()
                for d in range(vocab - 1):
                    send_v(d, g).wait_send()
                return carry

            lax.fori_loop(0, groups, drain_stats, 0)

        def dma(*shape):
            return pltpu.SemaphoreType.DMA(tuple(shape))

        anywhere = pl.BlockSpec(memory_space=pl.ANY)
        vmem = pl.BlockSpec(memory_space=pltpu.VMEM)
        return pl.pallas_call(
            kernel,
            out_shape=(
                pltpu.VMEM((tokens, draft), BF16),
                pltpu.VMEM((block, width), BF16),
                pltpu.VMEM((1, tokens), F32),
            ),
            in_specs=[anywhere] * 4 + [vmem],
            out_specs=(vmem,) * 3,
            scratch_shapes=[
                pltpu.VMEM((tokens, depth), BF16),
                pltpu.VMEM((tokens, depth), BF16),
                pltpu.VMEM((cores, depth, wc), BF16),
                pltpu.VMEM((tokens, draft), BF16),
                pltpu.VMEM((draft, width), BF16),
                pltpu.VMEM((draft, tokens), BF16),
                pltpu.VMEM((tokens, width), F32),
                pltpu.VMEM((tokens, half), F32),
                pltpu.VMEM((tokens, half), F32),
                pltpu.VMEM((tokens, half), BF16),
                pltpu.VMEM((tokens, half), BF16),
                pltpu.VMEM((groups, 8, gr), F32),
                pltpu.VMEM((groups, 8, gr), F32),
                pltpu.VMEM((groups, 8, gr), F32),
                pltpu.VMEM((vocab, groups, 8, gr), F32),
                pltpu.VMEM((tokens, 128), F32),
                pltpu.VMEM((tokens, width), BF16),
                pltpu.VMEM((chunks, sub, hc), BF16),
                pltpu.VMEM((chunks, sub, hc), BF16),
                pltpu.VMEM((chunks, gr, hc), F32),
                pltpu.VMEM((nz - 1, chunks, rz, hc), BF16),
                pltpu.VMEM((nz - 1, chunks, rz, hc), BF16),
                pltpu.VMEM((nx, block, width), BF16),
                pltpu.VMEM((nx, block, width), BF16),
                pltpu.VMEM((nx, block, width), F32),
                pltpu.VMEM((block, width), BF16),
                pltpu.VMEM((block, width), BF16),
            ]
            + [dma(groups), dma(groups), dma(2), dma(groups), dma(groups)]
            + [dma(total)] * 6
            + [dma(groups)] * 4
            + [dma(vocab - 1, groups)] * 2
            + [dma(chunks)] * 2
            + [dma(nz - 1, chunks)] * 4
            + [dma(chunks)] * 2
            + [dma(nx)] * 2
            + [dma(1)] * 2,
            compiler_params=pltpu.CompilerParams(
                collective_id=2, has_side_effects=True, vmem_limit_bytes=59 * 1024 * 1024
            ),
        )(th, tw, hd, wd, rw)

    def settle(*arrays):
        def kernel(*refs):
            n = len(arrays)
            copies = [
                pltpu.make_async_copy(refs[k], refs[n + k], refs[2 * n].at[k]) for k in range(n)
            ]
            for copy in copies:
                copy.start()
            for copy in copies:
                copy.wait()

        return pl.pallas_call(
            kernel,
            out_shape=tuple(jax.ShapeDtypeStruct(a.shape, a.dtype) for a in arrays),
            in_specs=[pl.BlockSpec(memory_space=pltpu.VMEM)] * len(arrays),
            out_specs=(pl.BlockSpec(memory_space=pl.ANY),) * len(arrays),
            scratch_shapes=[pltpu.SemaphoreType.DMA((len(arrays),))],
            compiler_params=pltpu.CompilerParams(vmem_limit_bytes=8 * 1024 * 1024),
        )(*arrays)

    def fits(th, tw, hd, wd):
        tokens, depth = th.shape
        paired = cores == 2 and nx == 2 and ny == 2 and nz == 4
        tiled = tokens == 4 * 128 and 128 % (ny * nz * 16) == 0 and depth % 4096 == 0
        room = tokens * depth * 4 + cores * depth * tw.shape[1] * 2 <= 24 * 2**20
        return paired and tiled and room

    def gathered(draft_hidden, teacher_hidden, draft_head, teacher_head, row_weight):
        grad_hidden, grad_head, kl = fused(
            teacher_hidden, teacher_head, draft_hidden, draft_head, row_weight.reshape(1, -1)
        )
        grad_hidden, grad_head, kl = settle(grad_hidden, grad_head, kl)
        return (grad_hidden, grad_head, kl.reshape(-1))

    def on_device(draft_hidden, teacher_hidden, draft_head, teacher_head, row_weight):
        if fits(teacher_hidden, teacher_head, draft_hidden, draft_head):
            return gathered(draft_hidden, teacher_hidden, draft_head, teacher_head, row_weight)
        row = lax.axis_index("rows")
        draft_logits = dot(draft_hidden, draft_head)
        draft_top = jnp.max(draft_logits, axis=1)
        draft_sum = jnp.sum(jnp.exp(draft_logits - draft_top[:, None]), axis=1)
        early = (draft_logits, draft_top, draft_sum, draft_hidden.T)
        teacher_logits, early = teacher(teacher_hidden, teacher_head, row, early)
        draft_logits, draft_top, draft_sum, hidden_t = early
        teach_top = jnp.max(teacher_logits, axis=1)
        teach_exp = jnp.exp(teacher_logits - teach_top[:, None])
        stats = jnp.stack(
            [
                draft_top,
                teach_top,
                draft_sum,
                jnp.sum(teach_exp, axis=1),
                jnp.sum(teach_exp * (teacher_logits - draft_logits), axis=1),
            ]
        )
        stats = swap_stats(stats)
        draft_top, teach_top = jnp.max(stats[:, 0], axis=0), jnp.max(stats[:, 1], axis=0)
        draft_scale = jnp.exp(stats[:, 0] - draft_top)
        teach_scale = jnp.exp(stats[:, 1] - teach_top)
        draft_sum = jnp.sum(stats[:, 2] * draft_scale, axis=0)
        teach_sum = jnp.sum(stats[:, 3] * teach_scale, axis=0)
        teach_gap = jnp.sum(stats[:, 4] * teach_scale, axis=0)
        draft_lse = draft_top + jnp.log(draft_sum)
        teacher_lse = teach_top + jnp.log(teach_sum)
        kl_rows = row_weight * (teach_gap / teach_sum - teacher_lse + draft_lse)
        teacher_prob = jnp.exp(teacher_logits - teacher_lse[:, None])
        draft_prob = jnp.exp(draft_logits - draft_lse[:, None])
        grad_logits = (row_weight[:, None] * (draft_prob - teacher_prob)).astype(BF16)
        grad_hidden, grad_head = sums(grad_logits, draft_head, hidden_t)
        return (grad_hidden, grad_head, kl_rows)

    return on_device


def solution(mesh):
    return jax.shard_map(
        make(mesh.shape["rows"], mesh.shape["vocab"]),
        mesh=mesh,
        in_specs=(
            P("rows", None),
            P("rows", None),
            P(None, "vocab"),
            P(None, ("vocab", "rows")),
            P("rows"),
        ),
        out_specs=(P("rows", None), P("rows", "vocab"), P("rows")),
        check_vma=False,
    )
```
